768 devices in a mesh: ta: 16 (over y, x_lo), sa: 48 (over x_hi, z, core).
Axes of the slice: x: 4 (x_hi: 2, x_lo: 2; x = x_hi * 2 + x_lo), y: 8, z: 12, core: 2. Of those that a mesh axis runs over, the one named last changes fastest.
Arguments:
- eigvecs: float32 [2, 32, 64, 3, 24576], P(None, 'ta', None, None, 'sa'), may hold values from -0.0234375 to 0.0234375
- solutions: float32 [2, 32, 3, 8, 4, 3, 24576], P(None, 'ta', None, None, None, None, 'sa'), may hold values from -15 to 15
- source_times: int32 [3], replicated, may hold values from 0 to 31, as said below
- spin_dilution: int32 [3, 8], replicated, may hold values from 0 to 3
Outputs:
- perambulator: float32 [2, 32, 6144], P(None, 'ta', 'sa')
- norms: float32 [3, 8], replicated
The draws below stay inside these ranges and needn't reach their ends.
Inputs may be any that keep to these rules, and one draw needn't show every extreme that they name: `source_times`: some source lies at slice 0 and another at slice 32 - 1.
All inputs are finite; a program needn't handle non-finite values.
Results may differ from the reference program's by a relative error of at most 0.000084.
Values sent between devices are 32-bit elements; how exact they have to be, the bound alone decides.
A program may use at most 32 MiB of HBM per device.

```python
import jax
import jax.numpy as jnp
from jax import lax

NEV = 64
NSRC = 3
COLS = 8
NT = 32
NSPACE = 24576


def times_for(key):
    base = jax.random.randint(jax.random.fold_in(key, 7), (NSRC,), 0, NT).astype(jnp.int32)
    last_pick = jax.random.randint(jax.random.fold_in(key, 8), (), 0, NSRC).astype(jnp.int32)
    step_pick = jax.random.randint(jax.random.fold_in(key, 9), (), 1, NSRC).astype(jnp.int32)
    first_pick = (last_pick + step_pick) % NSRC
    slots = jnp.arange(NSRC, dtype=jnp.int32)
    base = jnp.where(slots == last_pick, NT - 1, base)
    base = jnp.where(slots == first_pick, 0, base)
    return base.astype(jnp.int32)


def draw_source_times(key, part):
    return times_for(key)


def solution_part(key, salt):
    starts = times_for(key)
    slice_ids = jnp.arange(NT, dtype=jnp.int32)
    apart = jnp.abs(slice_ids[:, None] - starts[None, :])
    apart = jnp.minimum(apart, NT - apart).astype(jnp.float32)
    amplitude = 0.5 + 2.5 * jnp.exp(-apart * 16.0 / NT)
    shape = (NT, NSRC, COLS, 4, 3, NSPACE)
    noise_key = jax.random.fold_in(key, salt)
    noise = jnp.clip(jax.random.normal(noise_key, shape, jnp.float32), -5.0, 5.0)
    return noise * amplitude[:, :, None, None, None, None]


def draw_solutions(key, part):
    return jnp.stack([solution_part(key, 11), solution_part(key, 13)]).astype(jnp.float32)


def plant(entries, key, least, high):
    longest = entries.shape.index(max(entries.shape))
    spots = []
    for shift in (0, 1):
        where = [jax.random.randint(jax.random.fold_in(key, axis), (), 0, length) for axis, length in enumerate(entries.shape)]
        where[longest] = (where[longest] + shift) % entries.shape[longest]
        spots.append(tuple(where))
    return entries.at[spots[0]].set(least).at[spots[1]].set(high)


def level_of(stream_key, extent, shards, smallest, top_value):
    level = 1.0
    for dim, shards_of in shards:
        steps = jax.random.uniform(jax.random.fold_in(jax.random.fold_in(stream_key, 6), dim), (shards_of,), jnp.float32, smallest / len(shards), top_value / len(shards))
        level = level * jnp.repeat(jnp.exp(steps), extent[dim] // shards_of).reshape((-1,) + (1,) * (len(extent) - 1 - dim))
    return level


def centred(own_key, shape, width, bound, pieces=(), held_as=jnp.bfloat16):
    loudness = level_of(own_key, shape, pieces, -0.22, 0.18) if pieces else 1.0
    array = jax.random.normal(own_key, shape, jnp.float32) * width * loudness
    return jnp.minimum(jnp.maximum(array, -bound), bound).astype(held_as)


def setup_inputs(seed: int = 0) -> dict:
    seeds = jax.random.split(jax.random.key(seed), 5)
    eigvecs = centred(seeds[0], (2, NT, NEV, 3, NSPACE), (3 * NSPACE) ** -0.5, 0.0234375, ((1, 16), (4, 48)), jnp.float32)
    solutions = draw_solutions(jax.random.fold_in(seeds[4], 71), 0)
    source_times = draw_source_times(jax.random.fold_in(seeds[4], 71), 0)
    spin_dilution = plant(jax.random.randint(seeds[3], (NSRC, COLS), 0, 4), jax.random.fold_in(seeds[3], 1), 0, 3).astype(jnp.int32)
    return dict(eigvecs=eigvecs, solutions=solutions, source_times=source_times, spin_dilution=spin_dilution)


def slice_tile(inputs):
    eig_real, eig_imag, sol_real, sol_imag = inputs
    precise = lax.Precision.HIGHEST
    real_part = jnp.dot(eig_real, sol_real.T, precision=precise, preferred_element_type=jnp.float32) + jnp.dot(eig_imag, sol_imag.T, precision=precise, preferred_element_type=jnp.float32)
    imag_part = jnp.dot(eig_real, sol_imag.T, precision=precise, preferred_element_type=jnp.float32) - jnp.dot(eig_imag, sol_real.T, precision=precise, preferred_element_type=jnp.float32)
    return jnp.stack([real_part, imag_part])


def reference(eigvecs, solutions, source_times, spin_dilution):
    slice_count = eigvecs.shape[1]
    eig_count = eigvecs.shape[2]
    site_count = eigvecs.shape[4]
    src_count = spin_dilution.shape[0]
    col_count = spin_dilution.shape[1]
    columns = src_count * col_count * 4
    inner_len = 3 * site_count
    eigen_rows = eigvecs.reshape(2, slice_count, eig_count, inner_len)
    solution_rows = solutions.reshape(2, slice_count, columns, inner_len)
    tiles = lax.map(slice_tile, (eigen_rows[0], eigen_rows[1], solution_rows[0], solution_rows[1]))
    tiles = jnp.transpose(tiles, (1, 0, 2, 3))
    slice_times = jnp.arange(slice_count, dtype=jnp.int32)
    boundary = jnp.where(slice_times[:, None] < source_times[None, :], -1.0, 1.0).astype(jnp.float32)
    chirality = jnp.where(spin_dilution < 2, 1.0, -1.0).astype(jnp.float32)
    signs = jnp.broadcast_to((boundary[:, :, None] * chirality[None])[:, :, :, None], (slice_count, src_count, col_count, 4)).reshape(slice_count, columns)
    perambulator = (tiles * signs[None, :, None, :]).reshape(2, slice_count, eig_count * columns)
    norms = jnp.sum(solutions * solutions, axis=(0, 1, 4, 5, 6)) / (12.0 * slice_count * site_count)
    return perambulator, norms
```

```python
import jax
import jax.numpy as jnp
from jax import lax
from jax.experimental import pallas as pl
from jax.experimental.pallas import tpu as pltpu
from jax.sharding import Mesh
from jax.sharding import PartitionSpec as P

F32 = jnp.float32
BF16 = jnp.bfloat16
MESH = pl.DeviceIdType.MESH
NY, NXL, NXH, NZ, NC = 8, 2, 2, 12, 2
TA = ("y", "xl")
SA = ("xh", "z", "core")
NEAR = NZ * NC
PLANE = NXH * NY * NXL


def split(x):
    high = x.astype(BF16)
    low = (x - high.astype(F32)).astype(BF16)
    return high, low


def dot_rows(a, b):
    return lax.dot_general(a, b, (((1,), (1,)), ((), ())), preferred_element_type=F32)


def kernel(times_ref, spin_ref, eig_hbm, sol_hbm, out_ref, norm_ref,
           eig, sol, tmp, send, recv, half, other, nsend1, nrecv1, nsend2, nrecv2,
           load_sem, ssem, rsem):
    y, xl, xh = lax.axis_index("y"), lax.axis_index("xl"), lax.axis_index("xh")
    z, core = lax.axis_index("z"), lax.axis_index("core")
    near_id = z * NC + core
    plane_id = (xh * NY + y) * NXL + xl

    def loads(t):
        copies = []
        for p in range(2):
            copies.append(pltpu.make_async_copy(eig_hbm.at[p, t], eig.at[p, t], load_sem.at[t]))
            for c in range(3):
                for j in range(4):
                    copies.append(pltpu.make_async_copy(
                        sol_hbm.at[p, t, :, c, :, pl.ds(128 * j, 128)],
                        sol.at[p, t, c, j], load_sem.at[t]))
        return copies

    for t in range(2):
        for copy in loads(t):
            copy.start()

    def near_peer(i):
        d = lax.rem(near_id + i, NEAR)
        return {"z": d // NC, "core": lax.rem(d, NC)}

    def plane_peer(i):
        d = lax.rem(plane_id + i, PLANE)
        return {"xh": d // (NY * NXL), "y": lax.rem(d // NXL, NY), "xl": lax.rem(d, NXL)}

    barrier = pltpu.get_barrier_semaphore()

    @pl.loop(1, NEAR)
    def _(i):
        pl.semaphore_signal(barrier, inc=1, device_id=near_peer(i), device_id_type=MESH)

    @pl.loop(1, PLANE)
    def _(i):
        pl.semaphore_signal(barrier, inc=1, device_id=plane_peer(i), device_id_type=MESH)

    lane = lax.broadcasted_iota(jnp.int32, (1, 128), 1)
    signs = []
    for t in range(2):
        now = (y * NXL + xl) * 2 + t
        sign = jnp.ones((1, 128), F32)
        for s in range(3):
            edge = jnp.where(now < times_ref[s], F32(-1), F32(1))
            for k in range(8):
                chir = jnp.where(spin_ref[s, k] < 2, F32(1), F32(-1))
                sign = jnp.where(lane // 4 == s * 8 + k, edge * chir, sign)
        signs.append(sign)

    squares = jnp.zeros((96, 128), F32)
    lane16 = lax.broadcasted_iota(jnp.int32, (16, 128), 1)
    for t in range(2):
        for copy in loads(t):
            copy.wait()
        prod = jnp.zeros((128, 256), F32)
        for c in range(3):
            e = jnp.concatenate([eig[0, t, c], eig[1, t, c]], axis=0)
            rows = []
            for p in range(2):
                pieces = []
                for j in range(4):
                    piece = sol[p, t, c, j].reshape(96, 128)
                    squares = squares + piece * piece
                    pieces.append(piece)
                rows.append(jnp.concatenate(pieces, axis=1))
                rows.append(jnp.zeros((32, 512), F32))
            s = jnp.concatenate(rows, axis=0)
            eh, el = split(e)
            sh, sl = split(s)
            prod = prod + (dot_rows(eh, sh) + (dot_rows(eh, sl) + dot_rows(el, sh)))
        real = (prod[:64, :128] + prod[64:, 128:]) * signs[t]
        imag = (prod[:64, 128:] - prod[64:, :128]) * signs[t]
        for p, part in enumerate((real, imag)):
            tmp[...] = part
            a0 = tmp[pl.ds(0, 16, stride=4), :]
            r1 = pltpu.roll(tmp[pl.ds(1, 16, stride=4), :], 96, 1)
            r2 = pltpu.roll(tmp[pl.ds(2, 16, stride=4), :], 64, 1)
            r3 = pltpu.roll(tmp[pl.ds(3, 16, stride=4), :], 32, 1)
            blocks = (jnp.where(lane16 < 96, a0, r1), jnp.where(lane16 < 64, r1, r2),
                      jnp.where(lane16 < 32, r2, r3))
            for r, block in enumerate(blocks):
                for h in range(2):
                    send[pl.ds(r * 8 + h * 4 + p * 2 + t, 8, stride=24), :] = block[8 * h:8 * h + 8]

    total = jnp.sum(squares, axis=1, keepdims=True)
    row = lax.broadcasted_iota(jnp.int32, (96, 128), 0)
    col = lax.broadcasted_iota(jnp.int32, (96, 128), 1)
    nsend1[...] = jnp.sum(jnp.where(row // 4 == col, total, F32(0)), axis=0, keepdims=True)

    pl.semaphore_wait(barrier, NEAR - 1 + PLANE - 1)

    def near_norm(i):
        return pltpu.make_async_remote_copy(
            src_ref=nsend1, dst_ref=nrecv1.at[near_id], send_sem=ssem.at[0], recv_sem=rsem.at[0],
            device_id=near_peer(i), device_id_type=MESH)

    def near_block(i):
        peer = lax.rem(near_id + i, NEAR)
        return pltpu.make_async_remote_copy(
            src_ref=send.at[pl.ds(pl.multiple_of(peer * 8, 8), 8)], dst_ref=recv.at[near_id],
            send_sem=ssem.at[1], recv_sem=rsem.at[1],
            device_id=near_peer(i), device_id_type=MESH)

    def plane_norm(i):
        return pltpu.make_async_remote_copy(
            src_ref=nsend2, dst_ref=nrecv2.at[plane_id], send_sem=ssem.at[2], recv_sem=rsem.at[2],
            device_id=plane_peer(i), device_id_type=MESH)

    def middle_out(i, n):
        m = n // 2
        return m + jnp.where(lax.rem(i, 2) == 0, -(i // 2), (i + 1) // 2)

    @pl.loop(0, NEAR - 1)
    def _(i):
        near_norm(middle_out(i, NEAR)).start()

    @pl.loop(0, NEAR - 1)
    def _(i):
        near_block(middle_out(i, NEAR)).start()

    nrecv1[near_id] = nsend1[...]
    recv[near_id] = send[pl.ds(pl.multiple_of(near_id * 8, 8), 8), :]

    def arrived(buf, count, sem):
        pltpu.make_async_copy(buf.at[pl.ds(0, count)], buf.at[pl.ds(0, count)], sem).wait()

    arrived(nrecv1, NEAR - 1, rsem.at[0])
    nsend2[...] = jnp.sum(nrecv1[...], axis=0)

    @pl.loop(1, PLANE)
    def _(i):
        plane_norm(i).start()

    arrived(recv, NEAR - 1, rsem.at[1])
    block = jnp.sum(recv[...], axis=0)
    half[0] = block[:4]
    half[1] = block[4:]
    cross = pltpu.make_async_remote_copy(
        src_ref=half.at[1 - xh], dst_ref=other, send_sem=ssem.at[3], recv_sem=rsem.at[3],
        device_id={"xh": 1 - xh}, device_id_type=MESH)
    cross.start()
    nrecv2[plane_id] = nsend2[...]
    cross.wait()
    mine = half[xh] + other[...]
    out_ref[0] = mine[:2]
    out_ref[1] = mine[2:]

    arrived(nrecv2, PLANE - 1, rsem.at[2])
    norm = jnp.sum(nrecv2[...], axis=0) / F32(9437184.0)
    for s in range(3):
        norm_ref[s:s + 1, :] = pltpu.roll(norm, (128 - 8 * s) % 128, 1)[:, :8]

    arrived(nrecv1, NEAR - 1, ssem.at[0])
    arrived(recv, NEAR - 1, ssem.at[1])
    arrived(nrecv2, PLANE - 1, ssem.at[2])


def on_device(eigvecs, solutions, source_times, spin_dilution):
    eig = jnp.transpose(eigvecs, (0, 1, 3, 2, 4))
    sol = jnp.transpose(solutions, (0, 1, 2, 3, 5, 4, 6)).reshape(2, 2, 24, 3, 4, 512)
    vmem = pl.BlockSpec(memory_space=pltpu.VMEM)
    smem = pl.BlockSpec(memory_space=pltpu.SMEM)
    hbm = pl.BlockSpec(memory_space=pl.ANY)
    return pl.pallas_call(
        kernel,
        out_shape=(jax.ShapeDtypeStruct((2, 2, 128), F32), jax.ShapeDtypeStruct((3, 8), F32)),
        in_specs=[smem, smem, hbm, hbm],
        out_specs=(vmem, vmem),
        scratch_shapes=[
            pltpu.VMEM((2, 2, 3, 64, 512), F32),
            pltpu.VMEM((2, 2, 3, 4, 24, 4, 128), F32),
            pltpu.VMEM((64, 128), F32),
            pltpu.VMEM((NEAR * 8, 128), F32),
            pltpu.VMEM((NEAR, 8, 128), F32),
            pltpu.VMEM((2, 4, 128), F32),
            pltpu.VMEM((4, 128), F32),
            pltpu.VMEM((1, 128), F32),
            pltpu.VMEM((NEAR, 1, 128), F32),
            pltpu.VMEM((1, 128), F32),
            pltpu.VMEM((PLANE, 1, 128), F32),
            pltpu.SemaphoreType.DMA((2,)),
            pltpu.SemaphoreType.DMA((4,)),
            pltpu.SemaphoreType.DMA((4,)),
        ],
        compiler_params=pltpu.CompilerParams(collective_id=0, has_side_effects=True),
        name="perambulator",
    )(source_times, spin_dilution, eig, sol)


def solution(mesh):
    finer = Mesh(mesh.devices.reshape(NY, NXL, NXH, NZ, NC), TA + SA)
    return jax.shard_map(
        on_device,
        mesh=finer,
        in_specs=(P(None, TA, None, None, SA), P(None, TA, None, None, None, None, SA), P(), P()),
        out_specs=(P(None, TA, SA), P()),
        check_vma=False,
    )
```

```python
import jax
import jax.numpy as jnp
from jax import lax
from jax.experimental import pallas as pl
from jax.experimental.pallas import tpu as pltpu
from jax.sharding import Mesh
from jax.sharding import PartitionSpec as P

F32 = jnp.float32
BF16 = jnp.bfloat16
MESH = pl.DeviceIdType.MESH
NY, NXL, NXH, NZ, NC = 8, 2, 2, 12, 2
TA = ("y", "xl")
SA = ("xh", "z", "core")
COLUMN = NZ * NC
PLANE = NXH * NY * NXL


def split(x):
    high = x.astype(BF16)
    low = (x - high.astype(F32)).astype(BF16)
    return high, low


def dot_rows(a, b):
    return lax.dot_general(a, b, (((1,), (1,)), ((), ())), preferred_element_type=F32)


def kernel(times_ref, spin_ref, eig_hbm, sol_hbm, out_ref, norm_ref,
           eig, sol, tmp, send, recv, half, other, row, rows1, total, rows2, final,
           sol_sem, eig_sem, ssem, rsem, ready):
    y, xl, xh = lax.axis_index("y"), lax.axis_index("xl"), lax.axis_index("xh")
    z, core = lax.axis_index("z"), lax.axis_index("core")
    me = z * NC + 1 - core
    plane_me = (xh * NY + y) * NXL + xl
    is_root = me == 0

    def sol_loads(p, t):
        return [pltpu.make_async_copy(sol_hbm.at[p, t, :, c, :, pl.ds(128 * j, 128)],
                                      sol.at[p, t, c, j], sol_sem.at[p, t])
                for c in range(3) for j in range(4)]

    def eig_loads(t):
        return [pltpu.make_async_copy(eig_hbm.at[p, t], eig.at[p, t], eig_sem.at[t])
                for p in range(2)]

    for t in range(2):
        for p in range(2):
            for copy in sol_loads(p, t):
                copy.start()
    for t in range(2):
        for copy in eig_loads(t):
            copy.start()

    def column(o):
        return {"z": o // NC, "core": 1 - lax.rem(o, NC)}

    def plane(i):
        d = lax.rem(plane_me + i, PLANE)
        return {"xh": d // (NY * NXL), "y": lax.rem(d // NXL, NY), "xl": lax.rem(d, NXL)}

    barrier = pltpu.get_barrier_semaphore()

    @pl.loop(me + 1, COLUMN)
    def _(o):
        pl.semaphore_signal(barrier, inc=1, device_id=column(o), device_id_type=MESH)

    pl.semaphore_signal(barrier, inc=1, device_id={"xh": 1 - xh}, device_id_type=MESH)

    @pl.when(is_root)
    def _():
        @pl.loop(1, PLANE)
        def _(i):
            pl.semaphore_signal(barrier, inc=1, device_id=plane(i), device_id_type=MESH)

    squares = jnp.zeros((96, 128), F32)
    for t in range(2):
        for p in range(2):
            for copy in sol_loads(p, t):
                copy.wait()
            for c in range(3):
                for j in range(4):
                    piece = sol[p, t, c, j].reshape(96, 128)
                    squares = squares + piece * piece
        if t == 0:
            pl.semaphore_wait(barrier, me + 1 + jnp.where(is_root, PLANE - 1, 0))

            @pl.loop(0, me)
            def _(o):
                pl.semaphore_signal(ready, inc=1, device_id=column(o), device_id_type=MESH)

    sums = jnp.sum(squares, axis=1, keepdims=True)
    line = lax.broadcasted_iota(jnp.int32, (96, 128), 0)
    spot = lax.broadcasted_iota(jnp.int32, (96, 128), 1)
    row[...] = jnp.sum(jnp.where(line // 4 == spot, sums, F32(0)), axis=0, keepdims=True)

    up = pltpu.make_async_remote_copy(
        src_ref=row, dst_ref=rows1.at[me], send_sem=ssem.at[0], recv_sem=rsem.at[0],
        device_id={"z": 0, "core": 1}, device_id_type=MESH)

    @pl.when(jnp.logical_not(is_root))
    def _():
        up.start()

    lane = lax.broadcasted_iota(jnp.int32, (1, 128), 1)
    lane16 = lax.broadcasted_iota(jnp.int32, (16, 128), 1)
    for t in range(2):
        now = (y * NXL + xl) * 2 + t
        sign = jnp.ones((1, 128), F32)
        for s in range(3):
            edge = jnp.where(now < times_ref[s], F32(-1), F32(1))
            for k in range(8):
                chir = jnp.where(spin_ref[s, k] < 2, F32(1), F32(-1))
                sign = jnp.where(lane // 4 == s * 8 + k, edge * chir, sign)
        for copy in eig_loads(t):
            copy.wait()
        prod = jnp.zeros((128, 256), F32)
        for c in range(3):
            e = jnp.concatenate([eig[0, t, c], eig[1, t, c]], axis=0)
            parts = []
            for p in range(2):
                parts.append(jnp.concatenate(
                    [sol[p, t, c, j].reshape(96, 128) for j in range(4)], axis=1))
                parts.append(jnp.zeros((32, 512), F32))
            s = jnp.concatenate(parts, axis=0)
            eh, el = split(e)
            sh, sl = split(s)
            prod = prod + (dot_rows(eh, sh) + (dot_rows(eh, sl) + dot_rows(el, sh)))
        real = (prod[:64, :128] + prod[64:, 128:]) * sign
        imag = (prod[:64, 128:] - prod[64:, :128]) * sign
        for p, part in enumerate((real, imag)):
            tmp[...] = part
            a0 = tmp[pl.ds(0, 16, stride=4), :]
            r1 = pltpu.roll(tmp[pl.ds(1, 16, stride=4), :], 96, 1)
            r2 = pltpu.roll(tmp[pl.ds(2, 16, stride=4), :], 64, 1)
            r3 = pltpu.roll(tmp[pl.ds(3, 16, stride=4), :], 32, 1)
            blocks = (jnp.where(lane16 < 96, a0, r1), jnp.where(lane16 < 64, r1, r2),
                      jnp.where(lane16 < 32, r2, r3))
            for r, block in enumerate(blocks):
                for h in range(2):
                    send[pl.ds(r * 8 + h * 4 + p * 2 + t, 8, stride=24), :] = block[8 * h:8 * h + 8]

    def send_block(o):
        peer = column(o)
        place = pl.multiple_of((peer["z"] * NC + peer["core"]) * 8, 8)
        pltpu.make_async_remote_copy(
            src_ref=send.at[pl.ds(place, 8)], dst_ref=recv.at[me],
            send_sem=ssem.at[1], recv_sem=rsem.at[1],
            device_id=peer, device_id_type=MESH).start()

    @pl.loop(0, me)
    def _(o):
        send_block(o)

    @pl.when(me < COLUMN - 1)
    def _():
        pl.semaphore_wait(ready, COLUMN - 1 - me)

    @pl.loop(me + 1, COLUMN)
    def _(o):
        send_block(o)

    recv[me] = send[pl.ds(pl.multiple_of((z * NC + core) * 8, 8), 8), :]

    def arrived(buf, count, sem):
        pltpu.make_async_copy(buf.at[pl.ds(0, count)], buf.at[pl.ds(0, count)], sem).wait()

    @pl.when(is_root)
    def _():
        rows1[0] = row[...]
        arrived(rows1, COLUMN - 1, rsem.at[0])
        total[...] = jnp.sum(rows1[...], axis=0)

        @pl.loop(1, PLANE)
        def _(i):
            pltpu.make_async_remote_copy(
                src_ref=total, dst_ref=rows2.at[plane_me], send_sem=ssem.at[2], recv_sem=rsem.at[2],
                device_id=plane(i), device_id_type=MESH).start()

        rows2[plane_me] = total[...]

    arrived(recv, COLUMN - 1, rsem.at[1])
    block = jnp.sum(recv[...], axis=0)
    half[0] = block[:4]
    half[1] = block[4:]
    cross = pltpu.make_async_remote_copy(
        src_ref=half.at[1 - xh], dst_ref=other, send_sem=ssem.at[3], recv_sem=rsem.at[3],
        device_id={"xh": 1 - xh}, device_id_type=MESH)
    cross.start()
    cross.wait()
    mine = half[xh] + other[...]
    out_ref[0] = mine[:2]
    out_ref[1] = mine[2:]

    def down(o):
        return pltpu.make_async_remote_copy(
            src_ref=final, dst_ref=final, send_sem=ssem.at[4], recv_sem=rsem.at[4],
            device_id=column(o), device_id_type=MESH)

    @pl.when(is_root)
    def _():
        arrived(rows2, PLANE - 1, rsem.at[2])
        final[...] = jnp.sum(rows2[...], axis=0)

        @pl.loop(1, COLUMN)
        def _(o):
            down(o).start()

    @pl.when(jnp.logical_not(is_root))
    def _():
        down(0).wait_recv()

    norm = final[...] / F32(9437184.0)
    for s in range(3):
        norm_ref[s:s + 1, :] = pltpu.roll(norm, (128 - 8 * s) % 128, 1)[:, :8]

    arrived(recv, COLUMN - 1, ssem.at[1])

    @pl.when(is_root)
    def _():
        arrived(rows2, PLANE - 1, ssem.at[2])
        arrived(rows1, COLUMN - 1, ssem.at[4])

    @pl.when(jnp.logical_not(is_root))
    def _():
        up.wait_send()


def finish(block_ref, norm_ref, block_out, norm_out, sem):
    copies = [pltpu.make_async_copy(block_ref, block_out, sem.at[0]),
              pltpu.make_async_copy(norm_ref, norm_out, sem.at[1])]
    for copy in copies:
        copy.start()
    for copy in copies:
        copy.wait()


def on_device(eigvecs, solutions, source_times, spin_dilution):
    eig = jnp.transpose(eigvecs, (0, 1, 3, 2, 4))
    sol = jnp.transpose(solutions, (0, 1, 2, 3, 5, 4, 6)).reshape(2, 2, 24, 3, 4, 512)
    vmem = pl.BlockSpec(memory_space=pltpu.VMEM)
    smem = pl.BlockSpec(memory_space=pltpu.SMEM)
    hbm = pl.BlockSpec(memory_space=pl.ANY)
    results = (jax.ShapeDtypeStruct((2, 2, 128), F32), jax.ShapeDtypeStruct((3, 8), F32))
    block, norm = pl.pallas_call(
        kernel,
        out_shape=(pltpu.VMEM((2, 2, 128), F32), pltpu.VMEM((3, 8), F32)),
        in_specs=[smem, smem, hbm, hbm],
        out_specs=(vmem, vmem),
        scratch_shapes=[
            pltpu.VMEM((2, 2, 3, 64, 512), F32),
            pltpu.VMEM((2, 2, 3, 4, 24, 4, 128), F32),
            pltpu.VMEM((64, 128), F32),
            pltpu.VMEM((COLUMN * 8, 128), F32),
            pltpu.VMEM((COLUMN, 8, 128), F32),
            pltpu.VMEM((2, 4, 128), F32),
            pltpu.VMEM((4, 128), F32),
            pltpu.VMEM((1, 128), F32),
            pltpu.VMEM((COLUMN, 1, 128), F32),
            pltpu.VMEM((1, 128), F32),
            pltpu.VMEM((PLANE, 1, 128), F32),
            pltpu.VMEM((1, 128), F32),
            pltpu.SemaphoreType.DMA((2, 2)),
            pltpu.SemaphoreType.DMA((2,)),
            pltpu.SemaphoreType.DMA((5,)),
            pltpu.SemaphoreType.DMA((5,)),
            pltpu.SemaphoreType.REGULAR,
        ],
        compiler_params=pltpu.CompilerParams(collective_id=0, has_side_effects=True),
        name="perambulator",
    )(source_times, spin_dilution, eig, sol)
    return pl.pallas_call(
        finish,
        out_shape=results,
        in_specs=[vmem, vmem],
        out_specs=(hbm, hbm),
        scratch_shapes=[pltpu.SemaphoreType.DMA((2,))],
        compiler_params=pltpu.CompilerParams(vmem_limit_bytes=1 << 20),
        name="finish",
    )(pltpu.with_memory_space_constraint(block, pltpu.VMEM),
      pltpu.with_memory_space_constraint(norm, pltpu.VMEM))


def solution(mesh):
    finer = Mesh(mesh.devices.reshape(NY, NXL, NXH, NZ, NC), TA + SA)
    return jax.shard_map(
        on_device,
        mesh=finer,
        in_specs=(P(None, TA, None, None, SA), P(None, TA, None, None, None, None, SA), P(), P()),
        out_specs=(P(None, TA, SA), P()),
        check_vma=False,
    )
```

```python
import jax
import jax.numpy as jnp
from jax import lax
from jax.experimental import pallas as pl
from jax.experimental.pallas import tpu as pltpu
from jax.sharding import Mesh
from jax.sharding import PartitionSpec as P

F32 = jnp.float32
BF16 = jnp.bfloat16
MESH = pl.DeviceIdType.MESH
NY, NXL, NXH, NZ, NC = 8, 2, 2, 12, 2
TA = ("y", "xl")
SA = ("xh", "z", "core")
COLUMN = NZ * NC
PLANE = NXH * NY * NXL
LATE = 13


def split(x):
    high = x.astype(BF16)
    low = (x - high.astype(F32)).astype(BF16)
    return high, low


def dot_rows(a, b):
    return lax.dot_general(a, b, (((1,), (1,)), ((), ())), preferred_element_type=F32)


def kernel(times_hbm, spin_hbm, eig_hbm, sol_hbm, out_ref, norm_ref,
           eig, sol, times_ref, spin_ref, high, low, tmp, send, recv, half, other,
           row, rows1, total, rows2, final,
           sol_sem, eig_sem, int_sem, ssem, rsem, ready):
    y, xl, xh = lax.axis_index("y"), lax.axis_index("xl"), lax.axis_index("xh")
    z, core = lax.axis_index("z"), lax.axis_index("core")
    plane_me = (xh * NY + y) * NXL + xl
    place = z * NC + 1 - core
    first = plane_me == 0
    is_root = place == 0
    is_spare = jnp.logical_and(first, place == 1)
    shifted = jnp.where(place == 1, LATE, jnp.where(place <= LATE, place - 1, place))
    me = jnp.where(jnp.logical_and(first, place >= 1), shifted, place)

    def sol_load(p, t):
        return pltpu.make_async_copy(sol_hbm.at[p, t], sol.at[p, t], sol_sem.at[p, t])

    def eig_load(p, t):
        return pltpu.make_async_copy(eig_hbm.at[p, t], eig.at[p, t], eig_sem.at[p, t])

    for t in range(2):
        for p in range(2):
            sol_load(p, t).start()
    for t in range(2):
        for p in range(2):
            eig_load(p, t).start()

    int_loads = [pltpu.make_async_copy(times_hbm, times_ref, int_sem.at[0]),
                 pltpu.make_async_copy(spin_hbm, spin_ref, int_sem.at[1])]
    for copy in int_loads:
        copy.start()

    def at_place(n):
        return {"z": n // NC, "core": 1 - lax.rem(n, NC)}

    def column(o):
        moved = jnp.where(o == LATE, 1, jnp.where(o < LATE, o + 1, o))
        return at_place(jnp.where(jnp.logical_and(first, o >= 1), moved, o))

    def plane(d):
        return {"xh": d // (NY * NXL), "y": lax.rem(d // NXL, NY), "xl": lax.rem(d, NXL),
                "z": 0, "core": 1}

    def each_plane(action):
        @pl.loop(0, plane_me)
        def _(d):
            action(d)

        @pl.loop(plane_me + 1, PLANE)
        def _(d):
            action(d)

    barrier = pltpu.get_barrier_semaphore()

    def greet(device):
        pl.semaphore_signal(barrier, inc=1, device_id=device, device_id_type=MESH)

    @pl.loop(me + 1, COLUMN)
    def _(o):
        greet(column(o))

    greet({"xh": 1 - xh})

    @pl.when(is_root)
    def _():
        each_plane(lambda d: greet(plane(d)))

    @pl.when(is_spare)
    def _():
        @pl.loop(0, PLANE)
        def _(d):
            greet(plane(d))

    high[...] = jnp.zeros(high.shape, BF16)
    low[...] = jnp.zeros(low.shape, BF16)

    pl.semaphore_wait(barrier, me + 1 + jnp.where(is_root, PLANE, 0))

    @pl.loop(0, me)
    def _(o):
        pl.semaphore_signal(ready, inc=1, device_id=column(o), device_id_type=MESH)

    squares = jnp.zeros((24, 4, 512), F32)
    for t in range(2):
        for p in range(2):
            sol_load(p, t).wait()
            for c in range(3):
                piece = sol[p, t, :, c]
                squares = squares + piece * piece

    lanes = (squares[:, :, :128] + squares[:, :, 128:256]) + (squares[:, :, 256:384] + squares[:, :, 384:])
    sums = jnp.sum(lanes.reshape(96, 128), axis=1, keepdims=True)
    line = lax.broadcasted_iota(jnp.int32, (96, 128), 0)
    spot = lax.broadcasted_iota(jnp.int32, (96, 128), 1)
    row[...] = jnp.sum(jnp.where(line // 4 == spot, sums, F32(0)), axis=0, keepdims=True)

    up = pltpu.make_async_remote_copy(
        src_ref=row, dst_ref=rows1.at[me], send_sem=ssem.at[0], recv_sem=rsem.at[0],
        device_id={"z": 0, "core": 1}, device_id_type=MESH)

    @pl.when(jnp.logical_not(is_root))
    def _():
        up.start()

    for t in range(2):
        for p in range(2):
            for c in range(3):
                h, l = split(sol[p, t, :, c].reshape(96, 512))
                high[t, 128 * p:128 * p + 96, 512 * c:512 * c + 512] = h
                low[t, 128 * p:128 * p + 96, 512 * c:512 * c + 512] = l

    for copy in int_loads:
        copy.wait()
    lane = lax.broadcasted_iota(jnp.int32, (1, 128), 1)
    lane16 = lax.broadcasted_iota(jnp.int32, (16, 128), 1)
    signs = []
    for t in range(2):
        now = (y * NXL + xl) * 2 + t
        sign = jnp.ones((1, 128), F32)
        for s in range(3):
            edge = jnp.where(now < times_ref[s], F32(-1), F32(1))
            for k in range(8):
                chir = jnp.where(spin_ref[s, k] < 2, F32(1), F32(-1))
                sign = jnp.where(lane // 4 == s * 8 + k, edge * chir, sign)
        signs.append(sign)

    for t in range(2):
        sign = signs[t]
        eig_load(0, t).wait()
        eig_load(1, t).wait()
        e = jnp.concatenate(
            [jnp.concatenate([eig[p, t, c] for c in range(3)], axis=1) for p in range(2)], axis=0)
        eh, el = split(e)
        both = dot_rows(jnp.concatenate([eh, el], axis=0), high[t])
        prod = both[:128] + (both[128:] + dot_rows(eh, low[t]))
        real = (prod[:64, :128] + prod[64:, 128:]) * sign
        imag = (prod[:64, 128:] - prod[64:, :128]) * sign
        for p, part in enumerate((real, imag)):
            tmp[...] = part
            a0 = tmp[pl.ds(0, 16, stride=4), :]
            r1 = pltpu.roll(tmp[pl.ds(1, 16, stride=4), :], 96, 1)
            r2 = pltpu.roll(tmp[pl.ds(2, 16, stride=4), :], 64, 1)
            r3 = pltpu.roll(tmp[pl.ds(3, 16, stride=4), :], 32, 1)
            blocks = (jnp.where(lane16 < 96, a0, r1), jnp.where(lane16 < 64, r1, r2),
                      jnp.where(lane16 < 32, r2, r3))
            for r, block in enumerate(blocks):
                for h in range(2):
                    send[pl.ds(r * 8 + h * 4 + p * 2 + t, 8, stride=24), :] = block[8 * h:8 * h + 8]

    def send_block(o):
        peer = column(o)
        spot = pl.multiple_of((peer["z"] * NC + peer["core"]) * 8, 8)
        pltpu.make_async_remote_copy(
            src_ref=send.at[pl.ds(spot, 8)], dst_ref=recv.at[me],
            send_sem=ssem.at[1], recv_sem=rsem.at[1],
            device_id=peer, device_id_type=MESH).start()

    @pl.loop(0, me)
    def _(o):
        send_block(o)

    @pl.when(me < COLUMN - 1)
    def _():
        pl.semaphore_wait(ready, COLUMN - 1 - me)

    @pl.loop(me + 1, COLUMN)
    def _(o):
        send_block(o)

    recv[me] = send[pl.ds(pl.multiple_of((z * NC + core) * 8, 8), 8), :]

    def arrived(buf, count, sem):
        pltpu.make_async_copy(buf.at[pl.ds(0, count)], buf.at[pl.ds(0, count)], sem).wait()

    @pl.when(is_root)
    def _():
        rows1[0] = row[...]
        arrived(rows1, COLUMN - 1, rsem.at[0])
        total[...] = jnp.sum(rows1[...], axis=0)

        def share(device):
            pltpu.make_async_remote_copy(
                src_ref=total, dst_ref=rows2.at[plane_me], send_sem=ssem.at[2], recv_sem=rsem.at[2],
                device_id=device, device_id_type=MESH).start()

        @pl.when(jnp.logical_not(first))
        def _():
            share(plane(0))

        share({"xh": 0, "y": 0, "xl": 0, "z": 0, "core": 0})

        @pl.loop(1, plane_me)
        def _(d):
            share(plane(d))

        @pl.loop(plane_me + 1, PLANE)
        def _(d):
            share(plane(d))

        rows2[plane_me] = total[...]

    arrived(recv, COLUMN - 1, rsem.at[1])
    block = jnp.sum(recv[...], axis=0)
    half[0] = block[:4]
    half[1] = block[4:]
    cross = pltpu.make_async_remote_copy(
        src_ref=half.at[1 - xh], dst_ref=other, send_sem=ssem.at[3], recv_sem=rsem.at[3],
        device_id={"xh": 1 - xh}, device_id_type=MESH)
    cross.start()
    cross.wait()
    mine = half[xh] + other[...]
    out_ref[0] = mine[:2]
    out_ref[1] = mine[2:]

    def down(n):
        return pltpu.make_async_remote_copy(
            src_ref=final, dst_ref=final, send_sem=ssem.at[4], recv_sem=rsem.at[4],
            device_id=at_place(n), device_id_type=MESH)

    @pl.when(is_root)
    def _():
        arrived(rows2, PLANE - 1, rsem.at[2])

    @pl.when(is_spare)
    def _():
        arrived(rows2, PLANE, rsem.at[2])

    summing = jnp.logical_or(is_root, is_spare)

    @pl.when(summing)
    def _():
        final[...] = jnp.sum(rows2[...], axis=0)

    plain_root = jnp.logical_and(is_root, jnp.logical_not(first))

    @pl.when(plain_root)
    def _():
        @pl.loop(1, COLUMN)
        def _(n):
            down(n).start()

    @pl.when(is_spare)
    def _():
        @pl.loop(2, COLUMN)
        def _(n):
            down(n).start()

    @pl.when(jnp.logical_not(summing))
    def _():
        down(0).wait_recv()

    norm = final[...] / F32(9437184.0)
    for s in range(3):
        norm_ref[s:s + 1, :] = pltpu.roll(norm, (128 - 8 * s) % 128, 1)[:, :8]

    arrived(recv, COLUMN - 1, ssem.at[1])

    @pl.when(is_root)
    def _():
        arrived(rows2, PLANE, ssem.at[2])

    @pl.when(plain_root)
    def _():
        arrived(rows1, COLUMN - 1, ssem.at[4])

    @pl.when(is_spare)
    def _():
        arrived(rows1, COLUMN - 2, ssem.at[4])

    @pl.when(jnp.logical_not(is_root))
    def _():
        up.wait_send()


def finish(block_ref, norm_ref, block_out, norm_out, sem):
    copies = [pltpu.make_async_copy(block_ref, block_out, sem.at[0]),
              pltpu.make_async_copy(norm_ref, norm_out, sem.at[1])]
    for copy in copies:
        copy.start()
    for copy in copies:
        copy.wait()


def on_device(eigvecs, solutions, source_times, spin_dilution):
    eig = jnp.transpose(eigvecs, (0, 1, 3, 2, 4))
    sol = jnp.transpose(solutions, (0, 1, 2, 3, 5, 4, 6)).reshape(2, 2, 24, 3, 4, 512)
    vmem = pl.BlockSpec(memory_space=pltpu.VMEM)
    hbm = pl.BlockSpec(memory_space=pl.ANY)
    results = (jax.ShapeDtypeStruct((2, 2, 128), F32), jax.ShapeDtypeStruct((3, 8), F32))
    block, norm = pl.pallas_call(
        kernel,
        out_shape=(pltpu.VMEM((2, 2, 128), F32), pltpu.VMEM((3, 8), F32)),
        in_specs=[hbm, hbm, hbm, hbm],
        out_specs=(vmem, vmem),
        scratch_shapes=[
            pltpu.VMEM((2, 2, 3, 64, 512), F32),
            pltpu.VMEM((2, 2, 24, 3, 4, 512), F32),
            pltpu.SMEM((3,), jnp.int32),
            pltpu.SMEM((3, 8), jnp.int32),
            pltpu.VMEM((2, 256, 1536), BF16),
            pltpu.VMEM((2, 256, 1536), BF16),
            pltpu.VMEM((64, 128), F32),
            pltpu.VMEM((COLUMN * 8, 128), F32),
            pltpu.VMEM((COLUMN, 8, 128), F32),
            pltpu.VMEM((2, 4, 128), F32),
            pltpu.VMEM((4, 128), F32),
            pltpu.VMEM((1, 128), F32),
            pltpu.VMEM((COLUMN, 1, 128), F32),
            pltpu.VMEM((1, 128), F32),
            pltpu.VMEM((PLANE, 1, 128), F32),
            pltpu.VMEM((1, 128), F32),
            pltpu.SemaphoreType.DMA((2, 2)),
            pltpu.SemaphoreType.DMA((2, 2)),
            pltpu.SemaphoreType.DMA((2,)),
            pltpu.SemaphoreType.DMA((5,)),
            pltpu.SemaphoreType.DMA((5,)),
            pltpu.SemaphoreType.REGULAR,
        ],
        compiler_params=pltpu.CompilerParams(collective_id=0, has_side_effects=True),
        name="perambulator",
    )(source_times, spin_dilution, eig, sol)
    return pl.pallas_call(
        finish,
        out_shape=results,
        in_specs=[vmem, vmem],
        out_specs=(hbm, hbm),
        scratch_shapes=[pltpu.SemaphoreType.DMA((2,))],
        compiler_params=pltpu.CompilerParams(vmem_limit_bytes=1 << 20),
        name="finish",
    )(pltpu.with_memory_space_constraint(block, pltpu.VMEM),
      pltpu.with_memory_space_constraint(norm, pltpu.VMEM))


def solution(mesh):
    finer = Mesh(mesh.devices.reshape(NY, NXL, NXH, NZ, NC), TA + SA)
    return jax.shard_map(
        on_device,
        mesh=finer,
        in_specs=(P(None, TA, None, None, SA), P(None, TA, None, None, None, None, SA), P(), P()),
        out_specs=(P(None, TA, SA), P()),
        check_vma=False,
    )
```

```python
import functools

import jax
import jax.numpy as jnp
from jax import lax
from jax.experimental import pallas as pl
from jax.experimental.pallas import tpu as pltpu
from jax.sharding import Mesh
from jax.sharding import PartitionSpec as P

F32 = jnp.float32
BF16 = jnp.bfloat16
MESH = pl.DeviceIdType.MESH
NY, NXL, NXH, NZ, NC = 8, 2, 2, 12, 2
TA = ("y", "xl")
SA = ("xh", "z", "core")
COLUMN = NZ * NC
PLANE = NXH * NY * NXL
LATE = 13
GUESTS = 5
RELAY = 4
EARLY = (0, 1, 2, 16, 17)
FAR_Y, FAR_LO, FAR_HI = 4, 10, 20
FAR = FAR_HI - FAR_LO
DIRECT = NXH * NXL * FAR


def split(x):
    high = x.astype(BF16)
    low = (x - high.astype(F32)).astype(BF16)
    return high, low


def dot_rows(a, b):
    return lax.dot_general(a, b, (((1,), (1,)), ((), ())), preferred_element_type=F32)


def kernel(times_hbm, spin_hbm, eig_hbm, sol_hbm, out_ref, norm_ref,
           eig, sol, times_ref, spin_ref, high, low, tmp, send, recv, half, other,
           row, rows1, near, total, rows2, rows3, final,
           sol_sem, eig_sem, int_sem, ssem, rsem, ready):
    y, xl, xh = lax.axis_index("y"), lax.axis_index("xl"), lax.axis_index("xh")
    z, core = lax.axis_index("z"), lax.axis_index("core")
    plane_me = (xh * NY + y) * NXL + xl
    place = z * NC + 1 - core
    first = plane_me == 0
    is_root = place == 0
    is_guest = jnp.logical_and(first, jnp.logical_and(place >= 1, place <= GUESTS))
    is_spare = jnp.logical_and(first, place == 1)
    is_relay = jnp.logical_and(jnp.logical_not(first), place == RELAY)
    shifted = jnp.where(place == 1, LATE, jnp.where(place <= LATE, place - 1, place))
    me = jnp.where(jnp.logical_and(first, place >= 1), shifted, place)
    in_far = y == FAR_Y
    is_far = jnp.logical_and(in_far, jnp.logical_and(place >= FAR_LO, place < FAR_HI))
    is_early = jnp.logical_and(is_root, functools.reduce(
        jnp.logical_or, [plane_me == e for e in EARLY]))

    for q in range(4):
        pltpu.make_async_copy(sol_hbm.at[q % 2, q // 2], sol.at[q],
                              sol_sem.at[q // 3]).start()
    for q in range(4):
        pltpu.make_async_copy(eig_hbm.at[q % 2, q // 2], eig.at[q % 2, q // 2],
                              eig_sem).start()

    int_loads = [pltpu.make_async_copy(times_hbm, times_ref, int_sem.at[0]),
                 pltpu.make_async_copy(spin_hbm, spin_ref, int_sem.at[1])]
    for copy in int_loads:
        copy.start()

    def at_place(n):
        return {"z": n // NC, "core": 1 - lax.rem(n, NC)}

    def column(o):
        moved = jnp.where(o == LATE, 1, jnp.where(o < LATE, o + 1, o))
        return at_place(jnp.where(jnp.logical_and(first, o >= 1), moved, o))

    def plane_at(d):
        return {"xh": d // (NY * NXL), "y": d // NXL % NY, "xl": d % NXL, "z": 0, "core": 1}

    def plane(d):
        return {"xh": d // (NY * NXL), "y": lax.rem(d // NXL, NY), "xl": lax.rem(d, NXL),
                "z": 0, "core": 1}

    barrier = pltpu.get_barrier_semaphore()

    def greet(device):
        pl.semaphore_signal(barrier, inc=1, device_id=device, device_id_type=MESH)

    @pl.loop(me + 1, COLUMN)
    def _(o):
        greet(column(o))

    greet({"xh": 1 - xh})

    @pl.when(is_root)
    def _():
        @pl.loop(1, PLANE)
        def _(i):
            greet(plane(lax.rem(plane_me + i, PLANE)))

    @pl.when(is_guest)
    def _():
        @pl.loop(0, PLANE)
        def _(d):
            greet(plane(d))

    @pl.when(is_early)
    def _():
        @pl.loop(0, DIRECT)
        def _(i):
            n = FAR_LO + lax.rem(i, FAR)
            greet({"xh": i // (NXL * FAR), "xl": lax.rem(i // FAR, NXL), "y": FAR_Y,
                   "z": n // NC, "core": 1 - lax.rem(n, NC)})

    high[...] = jnp.zeros(high.shape, BF16)
    low[...] = jnp.zeros(low.shape, BF16)

    pl.semaphore_wait(barrier, me + 1 + jnp.where(is_root, PLANE - 1 + GUESTS, 0)
                      + jnp.where(is_far, len(EARLY), 0))

    @pl.loop(0, me)
    def _(o):
        pl.semaphore_signal(ready, inc=1, device_id=column(o), device_id_type=MESH)

    squares = jnp.zeros((24, 4, 512), F32)

    def arrived(buf, count, sem):
        pltpu.make_async_copy(buf.at[pl.ds(0, count)], buf.at[pl.ds(0, count)], sem).wait()

    for q in range(4):
        if q == 0:
            arrived(sol, 3, sol_sem.at[0])
        if q == 3:
            arrived(sol, 1, sol_sem.at[1])
        for c in range(3):
            piece = sol[q, :, c]
            squares = squares + piece * piece

    lanes = (squares[:, :, :128] + squares[:, :, 128:256]) + (squares[:, :, 256:384] + squares[:, :, 384:])
    sums = jnp.sum(lanes.reshape(96, 128), axis=1, keepdims=True)
    line = lax.broadcasted_iota(jnp.int32, (96, 128), 0)
    spot = lax.broadcasted_iota(jnp.int32, (96, 128), 1)
    row[...] = jnp.sum(jnp.where(line // 4 == spot, sums, F32(0)), axis=0, keepdims=True)

    def send_row(slot, sem, device):
        pltpu.make_async_remote_copy(
            src_ref=row, dst_ref=slot, send_sem=ssem, recv_sem=sem,
            device_id=device, device_id_type=MESH).start()

    @pl.when(is_far)
    def _():
        spot = (xh * NXL + xl) * FAR + place - FAR_LO
        for e in EARLY:
            send_row(rows3.at[spot], rsem.at[4], plane_at(e))
        send_row(rows1.at[me], rsem.at[4], {"z": 0, "core": 1})

    @pl.when(jnp.logical_not(jnp.logical_or(is_root, is_far)))
    def _():
        send_row(rows1.at[me], rsem.at[0], {"z": 0, "core": 1})

    for t in range(2):
        for p in range(2):
            for c in range(3):
                h, l = split(sol[2 * t + p, :, c].reshape(96, 512))
                high[t, 128 * p:128 * p + 96, 512 * c:512 * c + 512] = h
                low[t, 128 * p:128 * p + 96, 512 * c:512 * c + 512] = l

    for copy in int_loads:
        copy.wait()
    pltpu.make_async_copy(eig, eig, eig_sem).wait()
    lane = lax.broadcasted_iota(jnp.int32, (1, 128), 1)
    lane16 = lax.broadcasted_iota(jnp.int32, (16, 128), 1)
    signs = []
    for t in range(2):
        now = (y * NXL + xl) * 2 + t
        sign = jnp.ones((1, 128), F32)
        for s in range(3):
            edge = jnp.where(now < times_ref[s], F32(-1), F32(1))
            for k in range(8):
                chir = jnp.where(spin_ref[s, k] < 2, F32(1), F32(-1))
                sign = jnp.where(lane // 4 == s * 8 + k, edge * chir, sign)
        signs.append(sign)

    for t in range(2):
        sign = signs[t]
        e = jnp.concatenate(
            [jnp.concatenate([eig[p, t, c] for c in range(3)], axis=1) for p in range(2)], axis=0)
        eh, el = split(e)
        both = dot_rows(jnp.concatenate([eh, el], axis=0), high[t])
        prod = both[:128] + (both[128:] + dot_rows(eh, low[t]))
        real = (prod[:64, :128] + prod[64:, 128:]) * sign
        imag = (prod[:64, 128:] - prod[64:, :128]) * sign
        for p, part in enumerate((real, imag)):
            tmp[...] = part
            a0 = tmp[pl.ds(0, 16, stride=4), :]
            r1 = pltpu.roll(tmp[pl.ds(1, 16, stride=4), :], 96, 1)
            r2 = pltpu.roll(tmp[pl.ds(2, 16, stride=4), :], 64, 1)
            r3 = pltpu.roll(tmp[pl.ds(3, 16, stride=4), :], 32, 1)
            blocks = (jnp.where(lane16 < 96, a0, r1), jnp.where(lane16 < 64, r1, r2),
                      jnp.where(lane16 < 32, r2, r3))
            for r, block in enumerate(blocks):
                for h in range(2):
                    send[pl.ds(r * 8 + h * 4 + p * 2 + t, 8, stride=24), :] = block[8 * h:8 * h + 8]

    def send_block(o):
        peer = column(o)
        spot = pl.multiple_of((peer["z"] * NC + peer["core"]) * 8, 8)
        pltpu.make_async_remote_copy(
            src_ref=send.at[pl.ds(spot, 8)], dst_ref=recv.at[me],
            send_sem=ssem, recv_sem=rsem.at[1],
            device_id=peer, device_id_type=MESH).start()

    @pl.loop(0, me)
    def _(o):
        send_block(o)

    @pl.when(me < COLUMN - 1)
    def _():
        pl.semaphore_wait(ready, COLUMN - 1 - me)

    @pl.loop(me + 1, COLUMN)
    def _(o):
        send_block(o)

    recv[me] = send[pl.ds(pl.multiple_of((z * NC + core) * 8, 8), 8), :]

    def share(source, device):
        pltpu.make_async_remote_copy(
            src_ref=source, dst_ref=rows2.at[plane_me], send_sem=ssem, recv_sem=rsem.at[2],
            device_id=device, device_id_type=MESH).start()

    def share_early(source):
        for e in EARLY:
            @pl.when(plane_me != e)
            def _():
                share(source, plane_at(e))

    @pl.when(is_root)
    def _():
        rows1[0] = row[...]

    @pl.when(jnp.logical_and(is_root, in_far))
    def _():
        arrived(rows1, COLUMN - 1 - FAR, rsem.at[0])
        near[...] = (jnp.sum(rows1[0:FAR_LO], axis=0)
                     + jnp.sum(rows1[FAR_HI:COLUMN], axis=0))
        share_early(near)
        arrived(rows1, FAR, rsem.at[4])
        total[...] = near[...] + jnp.sum(rows1[FAR_LO:FAR_HI], axis=0)

    @pl.when(jnp.logical_and(is_root, jnp.logical_not(in_far)))
    def _():
        arrived(rows1, COLUMN - 1, rsem.at[0])
        total[...] = jnp.sum(rows1[0:COLUMN], axis=0)
        share_early(total)

    @pl.when(is_root)
    def _():
        for n in range(1, GUESTS + 1):
            share(total, {"xh": 0, "y": 0, "xl": 0, "z": n // NC, "core": 1 - n % NC})

        for low_end, high_end in ((3, 16), (18, 32)):
            @pl.loop(low_end, high_end)
            def _(d):
                @pl.when(d != plane_me)
                def _():
                    share(total, plane(d))

        rows2[plane_me] = total[...]

    arrived(recv, COLUMN - 1, rsem.at[1])
    block = jnp.sum(recv[...], axis=0)
    half[0] = block[:4]
    half[1] = block[4:]
    cross = pltpu.make_async_remote_copy(
        src_ref=half.at[1 - xh], dst_ref=other, send_sem=ssem, recv_sem=rsem.at[3],
        device_id={"xh": 1 - xh}, device_id_type=MESH)
    cross.start()
    cross.wait_recv()
    mine = half[xh] + other[...]
    out_ref[0] = mine[:2]
    out_ref[1] = mine[2:]

    def down(n):
        return pltpu.make_async_remote_copy(
            src_ref=final, dst_ref=final, send_sem=ssem, recv_sem=rsem.at[0],
            device_id=at_place(n), device_id_type=MESH)

    @pl.when(is_root)
    def _():
        arrived(rows2, PLANE - 1, rsem.at[2])

    @pl.when(is_guest)
    def _():
        arrived(rows2, PLANE, rsem.at[2])

    summing = jnp.logical_or(is_root, is_guest)

    @pl.when(summing)
    def _():
        final[...] = jnp.sum(rows2[...], axis=0)

    @pl.when(is_early)
    def _():
        arrived(rows3, DIRECT, rsem.at[4])
        final[...] = final[...] + jnp.sum(rows3[...], axis=0)

    @pl.when(jnp.logical_not(summing))
    def _():
        down(0).wait_recv()

    plain_root = jnp.logical_and(is_root, jnp.logical_not(first))

    @pl.when(plain_root)
    def _():
        for n in range(1, RELAY + 1):
            down(n).start()

    @pl.when(is_relay)
    def _():
        @pl.loop(RELAY + 1, COLUMN)
        def _(n):
            down(n).start()

    @pl.when(is_spare)
    def _():
        @pl.loop(GUESTS + 1, COLUMN)
        def _(n):
            down(n).start()

    norm = final[...] / F32(9437184.0)
    for s in range(3):
        norm_ref[s:s + 1, :] = pltpu.roll(norm, (128 - 8 * s) % 128, 1)[:, :8]

    base = 8 * (COLUMN - 1) + 4
    roles = ((jnp.logical_and(is_root, first), PLANE - 1 + GUESTS),
             (plain_root, PLANE - 1 + GUESTS + RELAY),
             (is_relay, COLUMN - RELAY),
             (is_spare, COLUMN - GUESTS),
             (is_far, 1 + len(EARLY)))
    rest = True
    for role, count in roles:
        pl.when(role)(functools.partial(arrived, rows1, base + count, ssem))
        rest = jnp.logical_and(rest, jnp.logical_not(role))
    pl.when(rest)(functools.partial(arrived, rows1, base + 1, ssem))


def finish(block_ref, norm_ref, block_out, norm_out, sem):
    copies = [pltpu.make_async_copy(block_ref, block_out, sem.at[0]),
              pltpu.make_async_copy(norm_ref, norm_out, sem.at[1])]
    for copy in copies:
        copy.start()
    for copy in copies:
        copy.wait()


def on_device(eigvecs, solutions, source_times, spin_dilution):
    eig = jnp.transpose(eigvecs, (0, 1, 3, 2, 4))
    sol = jnp.transpose(solutions, (0, 1, 2, 3, 5, 4, 6)).reshape(2, 2, 24, 3, 4, 512)
    vmem = pl.BlockSpec(memory_space=pltpu.VMEM)
    hbm = pl.BlockSpec(memory_space=pl.ANY)
    results = (jax.ShapeDtypeStruct((2, 2, 128), F32), jax.ShapeDtypeStruct((3, 8), F32))
    block, norm = pl.pallas_call(
        kernel,
        out_shape=(pltpu.VMEM((2, 2, 128), F32), pltpu.VMEM((3, 8), F32)),
        in_specs=[hbm, hbm, hbm, hbm],
        out_specs=(vmem, vmem),
        scratch_shapes=[
            pltpu.VMEM((2, 2, 3, 64, 512), F32),
            pltpu.VMEM((4, 24, 3, 4, 512), F32),
            pltpu.SMEM((3,), jnp.int32),
            pltpu.SMEM((3, 8), jnp.int32),
            pltpu.VMEM((2, 256, 1536), BF16),
            pltpu.VMEM((2, 256, 1536), BF16),
            pltpu.VMEM((64, 128), F32),
            pltpu.VMEM((COLUMN * 8, 128), F32),
            pltpu.VMEM((COLUMN, 8, 128), F32),
            pltpu.VMEM((2, 4, 128), F32),
            pltpu.VMEM((4, 128), F32),
            pltpu.VMEM((1, 128), F32),
            pltpu.VMEM((256, 1, 128), F32),
            pltpu.VMEM((1, 128), F32),
            pltpu.VMEM((1, 128), F32),
            pltpu.VMEM((PLANE, 1, 128), F32),
            pltpu.VMEM((DIRECT, 1, 128), F32),
            pltpu.VMEM((1, 128), F32),
            pltpu.SemaphoreType.DMA((2,)),
            pltpu.SemaphoreType.DMA,
            pltpu.SemaphoreType.DMA((2,)),
            pltpu.SemaphoreType.DMA,
            pltpu.SemaphoreType.DMA((5,)),
            pltpu.SemaphoreType.REGULAR,
        ],
        compiler_params=pltpu.CompilerParams(collective_id=0, has_side_effects=True),
        name="perambulator",
    )(source_times, spin_dilution, eig, sol)
    return pl.pallas_call(
        finish,
        out_shape=results,
        in_specs=[vmem, vmem],
        out_specs=(hbm, hbm),
        scratch_shapes=[pltpu.SemaphoreType.DMA((2,))],
        compiler_params=pltpu.CompilerParams(vmem_limit_bytes=1 << 20),
        name="finish",
    )(pltpu.with_memory_space_constraint(block, pltpu.VMEM),
      pltpu.with_memory_space_constraint(norm, pltpu.VMEM))


def solution(mesh):
    finer = Mesh(mesh.devices.reshape(NY, NXL, NXH, NZ, NC), TA + SA)
    return jax.shard_map(
        on_device,
        mesh=finer,
        in_specs=(P(None, TA, None, None, SA), P(None, TA, None, None, None, None, SA), P(), P()),
        out_specs=(P(None, TA, SA), P()),
        check_vma=False,
    )
```

```python
import functools

import jax
import jax.numpy as jnp
from jax import lax
from jax.experimental import pallas as pl
from jax.experimental.pallas import tpu as pltpu
from jax.sharding import Mesh
from jax.sharding import PartitionSpec as P

F32 = jnp.float32
BF16 = jnp.bfloat16
MESH = pl.DeviceIdType.MESH
NY, NXL, NXH, NZ, NC = 8, 2, 2, 12, 2
TA = ("y", "xl")
SA = ("xh", "z", "core")
COLUMN = NZ * NC
PLANE = NXH * NY * NXL
LATE = 13
GUESTS = 7
RELAY = 4
EARLY = (0, 1, 2, 16, 17)
FAR_Y, FAR_YS, FAR_LO = 4, 2, 10
FAR = COLUMN - FAR_LO
DIRECT = NXH * NXL * FAR_YS * FAR


def split(x):
    high = x.astype(BF16)
    low = (x - high.astype(F32)).astype(BF16)
    return high, low


def dot_rows(a, b):
    return lax.dot_general(a, b, (((1,), (1,)), ((), ())), preferred_element_type=F32)


def kernel(times_hbm, spin_hbm, eig_hbm, sol_hbm, out_ref, norm_ref,
           eig, sol, times_ref, spin_ref, high, low, tmp, send, recv, half, other,
           row, rows1, near, total, rows2, rows3, final,
           sol_sem, eig_sem, int_sem, ssem, rsem, ready):
    y, xl, xh = lax.axis_index("y"), lax.axis_index("xl"), lax.axis_index("xh")
    z, core = lax.axis_index("z"), lax.axis_index("core")
    plane_me = (xh * NY + y) * NXL + xl
    place = z * NC + 1 - core
    first = plane_me == 0
    is_root = place == 0
    is_guest = jnp.logical_and(first, jnp.logical_and(place >= 1, place <= GUESTS))
    is_spare = jnp.logical_and(first, place == 1)
    is_relay = jnp.logical_and(jnp.logical_not(first), place == RELAY)
    shifted = jnp.where(place == 1, LATE, jnp.where(place <= LATE, place - 1, place))
    me = jnp.where(jnp.logical_and(first, place >= 1), shifted, place)
    in_far = jnp.logical_and(y >= FAR_Y, y < FAR_Y + FAR_YS)
    is_far = jnp.logical_and(in_far, place >= FAR_LO)
    is_early = jnp.logical_and(is_root, functools.reduce(
        jnp.logical_or, [plane_me == e for e in EARLY]))

    for q in range(4):
        pltpu.make_async_copy(sol_hbm.at[q % 2, q // 2], sol.at[q],
                              sol_sem.at[q // 3]).start()
    for q in range(4):
        pltpu.make_async_copy(eig_hbm.at[q % 2, q // 2], eig.at[q % 2, q // 2],
                              eig_sem).start()

    int_loads = [pltpu.make_async_copy(times_hbm, times_ref, int_sem.at[0]),
                 pltpu.make_async_copy(spin_hbm, spin_ref, int_sem.at[1])]
    for copy in int_loads:
        copy.start()

    def at_place(n):
        return {"z": n // NC, "core": 1 - lax.rem(n, NC)}

    def column(o):
        moved = jnp.where(o == LATE, 1, jnp.where(o < LATE, o + 1, o))
        return at_place(jnp.where(jnp.logical_and(first, o >= 1), moved, o))

    def plane_at(d):
        return {"xh": d // (NY * NXL), "y": d // NXL % NY, "xl": d % NXL, "z": 0, "core": 1}

    def plane(d):
        return {"xh": d // (NY * NXL), "y": lax.rem(d // NXL, NY), "xl": lax.rem(d, NXL),
                "z": 0, "core": 1}

    barrier = pltpu.get_barrier_semaphore()

    def greet(device):
        pl.semaphore_signal(barrier, inc=1, device_id=device, device_id_type=MESH)

    @pl.loop(me + 1, COLUMN)
    def _(o):
        greet(column(o))

    greet({"xh": 1 - xh})

    @pl.when(is_root)
    def _():
        @pl.loop(1, PLANE)
        def _(i):
            greet(plane(lax.rem(plane_me + i, PLANE)))

    @pl.when(is_guest)
    def _():
        @pl.loop(0, PLANE)
        def _(d):
            greet(plane(d))

    @pl.when(is_early)
    def _():
        @pl.loop(0, DIRECT)
        def _(i):
            n = FAR_LO + lax.rem(i, FAR)
            greet({"xh": i // (NXL * FAR_YS * FAR), "xl": lax.rem(i // (FAR_YS * FAR), NXL),
                   "y": FAR_Y + lax.rem(i // FAR, FAR_YS),
                   "z": n // NC, "core": 1 - lax.rem(n, NC)})

    high[...] = jnp.zeros(high.shape, BF16)
    low[...] = jnp.zeros(low.shape, BF16)

    pl.semaphore_wait(barrier, me + 1 + jnp.where(is_root, PLANE - 1 + GUESTS, 0)
                      + jnp.where(is_far, len(EARLY), 0))

    @pl.loop(0, me)
    def _(o):
        pl.semaphore_signal(ready, inc=1, device_id=column(o), device_id_type=MESH)

    squares = jnp.zeros((24, 4, 512), F32)

    def arrived(buf, count, sem):
        pltpu.make_async_copy(buf.at[pl.ds(0, count)], buf.at[pl.ds(0, count)], sem).wait()

    for q in range(4):
        if q == 0:
            arrived(sol, 3, sol_sem.at[0])
        if q == 3:
            arrived(sol, 1, sol_sem.at[1])
        for c in range(3):
            piece = sol[q, :, c]
            squares = squares + piece * piece

    lanes = (squares[:, :, :128] + squares[:, :, 128:256]) + (squares[:, :, 256:384] + squares[:, :, 384:])
    sums = jnp.sum(lanes.reshape(96, 128), axis=1, keepdims=True)
    line = lax.broadcasted_iota(jnp.int32, (96, 128), 0)
    spot = lax.broadcasted_iota(jnp.int32, (96, 128), 1)
    row[...] = jnp.sum(jnp.where(line // 4 == spot, sums, F32(0)), axis=0, keepdims=True)

    def send_row(slot, sem, device):
        pltpu.make_async_remote_copy(
            src_ref=row, dst_ref=slot, send_sem=ssem, recv_sem=sem,
            device_id=device, device_id_type=MESH).start()

    @pl.when(is_far)
    def _():
        spot = ((xh * NXL + xl) * FAR_YS + y - FAR_Y) * FAR + place - FAR_LO
        send_row(rows3.at[spot], rsem.at[4], plane_at(EARLY[0]))
        send_row(rows1.at[me], rsem.at[4], {"z": 0, "core": 1})
        for e in EARLY[1:]:
            send_row(rows3.at[spot], rsem.at[4], plane_at(e))

    @pl.when(jnp.logical_not(jnp.logical_or(is_root, is_far)))
    def _():
        send_row(rows1.at[me], rsem.at[0], {"z": 0, "core": 1})

    for t in range(2):
        for p in range(2):
            for c in range(3):
                h, l = split(sol[2 * t + p, :, c].reshape(96, 512))
                high[t, 128 * p:128 * p + 96, 512 * c:512 * c + 512] = h
                low[t, 128 * p:128 * p + 96, 512 * c:512 * c + 512] = l

    for copy in int_loads:
        copy.wait()
    pltpu.make_async_copy(eig, eig, eig_sem).wait()
    lane = lax.broadcasted_iota(jnp.int32, (1, 128), 1)
    lane16 = lax.broadcasted_iota(jnp.int32, (16, 128), 1)
    signs = []
    for t in range(2):
        now = (y * NXL + xl) * 2 + t
        sign = jnp.ones((1, 128), F32)
        for s in range(3):
            edge = jnp.where(now < times_ref[s], F32(-1), F32(1))
            for k in range(8):
                chir = jnp.where(spin_ref[s, k] < 2, F32(1), F32(-1))
                sign = jnp.where(lane // 4 == s * 8 + k, edge * chir, sign)
        signs.append(sign)

    for t in range(2):
        sign = signs[t]
        e = jnp.concatenate(
            [jnp.concatenate([eig[p, t, c] for c in range(3)], axis=1) for p in range(2)], axis=0)
        eh, el = split(e)
        both = dot_rows(jnp.concatenate([eh, el], axis=0), high[t])
        prod = both[:128] + (both[128:] + dot_rows(eh, low[t]))
        real = (prod[:64, :128] + prod[64:, 128:]) * sign
        imag = (prod[:64, 128:] - prod[64:, :128]) * sign
        for p, part in enumerate((real, imag)):
            tmp[:64] = part
            a0 = tmp[pl.ds(0, 16, stride=4), :]
            r1 = pltpu.roll(tmp[pl.ds(1, 16, stride=4), :], 96, 1)
            r2 = pltpu.roll(tmp[pl.ds(2, 16, stride=4), :], 64, 1)
            r3 = pltpu.roll(tmp[pl.ds(3, 16, stride=4), :], 32, 1)
            blocks = (jnp.where(lane16 < 96, a0, r1), jnp.where(lane16 < 64, r1, r2),
                      jnp.where(lane16 < 32, r2, r3))
            for r, block in enumerate(blocks):
                for h in range(2):
                    send[pl.ds(r * 8 + h * 4 + p * 2 + t, 8, stride=24), :] = block[8 * h:8 * h + 8]

    def send_block(o):
        peer = column(o)
        spot = pl.multiple_of((peer["z"] * NC + peer["core"]) * 8, 8)
        pltpu.make_async_remote_copy(
            src_ref=send.at[pl.ds(spot, 8)], dst_ref=recv.at[me],
            send_sem=ssem, recv_sem=rsem.at[1],
            device_id=peer, device_id_type=MESH).start()

    @pl.loop(0, me)
    def _(o):
        send_block(o)

    def share(source, device):
        pltpu.make_async_remote_copy(
            src_ref=source, dst_ref=rows2.at[plane_me], send_sem=ssem, recv_sem=rsem.at[2],
            device_id=device, device_id_type=MESH).start()

    def share_early(source):
        for e in EARLY:
            @pl.when(plane_me != e)
            def _():
                share(source, plane_at(e))

    is_far_root = jnp.logical_and(is_root, in_far)

    @pl.when(is_root)
    def _():
        rows1[0] = row[...]

    @pl.when(is_far_root)
    def _():
        arrived(rows1, FAR_LO - 1, rsem.at[0])
        near[...] = jnp.sum(rows1[0:FAR_LO], axis=0)
        share_early(near)

    @pl.when(me < COLUMN - 1)
    def _():
        pl.semaphore_wait(ready, COLUMN - 1 - me)

    @pl.loop(me + 1, COLUMN)
    def _(o):
        send_block(o)

    recv[me] = send[pl.ds(pl.multiple_of((z * NC + core) * 8, 8), 8), :]

    @pl.when(is_far_root)
    def _():
        arrived(rows1, FAR, rsem.at[4])
        total[...] = near[...] + jnp.sum(rows1[FAR_LO:COLUMN], axis=0)

    @pl.when(jnp.logical_and(is_root, jnp.logical_not(in_far)))
    def _():
        arrived(rows1, COLUMN - 1, rsem.at[0])
        total[...] = jnp.sum(rows1[0:COLUMN], axis=0)
        share_early(total)

    @pl.when(is_root)
    def _():
        for n in range(1, GUESTS + 1):
            share(total, {"xh": 0, "y": 0, "xl": 0, "z": n // NC, "core": 1 - n % NC})

        for low_end, high_end in ((3, 16), (18, 32)):
            @pl.loop(low_end, high_end)
            def _(d):
                @pl.when(d != plane_me)
                def _():
                    share(total, plane(d))

        rows2[plane_me] = total[...]

    arrived(recv, COLUMN - 1, rsem.at[1])
    block = jnp.sum(recv[...], axis=0)
    half[0] = block[:4]
    half[1] = block[4:]
    cross = pltpu.make_async_remote_copy(
        src_ref=half.at[1 - xh], dst_ref=other, send_sem=ssem, recv_sem=rsem.at[3],
        device_id={"xh": 1 - xh}, device_id_type=MESH)
    cross.start()
    cross.wait_recv()
    mine = half[xh] + other[...]
    out_ref[0] = mine[:2]
    out_ref[1] = mine[2:]

    def down(n):
        return pltpu.make_async_remote_copy(
            src_ref=final, dst_ref=final, send_sem=ssem, recv_sem=rsem.at[0],
            device_id=at_place(n), device_id_type=MESH)

    @pl.when(is_root)
    def _():
        arrived(rows2, PLANE - 1, rsem.at[2])

    @pl.when(is_guest)
    def _():
        arrived(rows2, PLANE, rsem.at[2])

    summing = jnp.logical_or(is_root, is_guest)

    @pl.when(summing)
    def _():
        final[...] = jnp.sum(rows2[...], axis=0)

    @pl.when(is_early)
    def _():
        arrived(rows3, DIRECT, rsem.at[4])
        final[...] = final[...] + jnp.sum(rows3[...], axis=0)

    @pl.when(jnp.logical_not(summing))
    def _():
        down(0).wait_recv()

    plain_root = jnp.logical_and(is_root, jnp.logical_not(first))

    @pl.when(plain_root)
    def _():
        for n in range(1, RELAY + 1):
            down(n).start()

    @pl.when(is_relay)
    def _():
        @pl.loop(RELAY + 1, COLUMN)
        def _(n):
            down(n).start()

    @pl.when(is_spare)
    def _():
        @pl.loop(GUESTS + 1, COLUMN)
        def _(n):
            down(n).start()

    norm = final[...] / F32(9437184.0)
    for s in range(3):
        norm_ref[s:s + 1, :] = pltpu.roll(norm, (128 - 8 * s) % 128, 1)[:, :8]

    base = 8 * (COLUMN - 1) + 4
    roles = ((jnp.logical_and(is_root, first), PLANE - 1 + GUESTS),
             (plain_root, PLANE - 1 + GUESTS + RELAY),
             (is_relay, COLUMN - RELAY),
             (is_spare, COLUMN - GUESTS),
             (is_far, 1 + len(EARLY)))
    rest = True
    for role, count in roles:
        pl.when(role)(functools.partial(arrived, rows1, base + count, ssem))
        rest = jnp.logical_and(rest, jnp.logical_not(role))
    pl.when(rest)(functools.partial(arrived, rows1, base + 1, ssem))


def finish(block_ref, norm_ref, block_out, norm_out, sem):
    copies = [pltpu.make_async_copy(block_ref, block_out, sem.at[0]),
              pltpu.make_async_copy(norm_ref, norm_out, sem.at[1])]
    for copy in copies:
        copy.start()
    for copy in copies:
        copy.wait()


def on_device(eigvecs, solutions, source_times, spin_dilution):
    eig = jnp.transpose(eigvecs, (0, 1, 3, 2, 4))
    sol = jnp.transpose(solutions, (0, 1, 2, 3, 5, 4, 6)).reshape(2, 2, 24, 3, 4, 512)
    vmem = pl.BlockSpec(memory_space=pltpu.VMEM)
    hbm = pl.BlockSpec(memory_space=pl.ANY)
    results = (jax.ShapeDtypeStruct((2, 2, 128), F32), jax.ShapeDtypeStruct((3, 8), F32))
    block, norm = pl.pallas_call(
        kernel,
        out_shape=(pltpu.VMEM((2, 2, 128), F32), pltpu.VMEM((3, 8), F32)),
        in_specs=[hbm, hbm, hbm, hbm],
        out_specs=(vmem, vmem),
        scratch_shapes=[
            pltpu.VMEM((2, 2, 3, 64, 512), F32),
            pltpu.VMEM((4, 24, 3, 4, 512), F32),
            pltpu.SMEM((3,), jnp.int32),
            pltpu.SMEM((3, 8), jnp.int32),
            pltpu.VMEM((2, 256, 1536), BF16),
            pltpu.VMEM((2, 256, 1536), BF16),
            pltpu.VMEM((72, 128), F32),
            pltpu.VMEM((COLUMN * 8 + 24, 128), F32),
            pltpu.VMEM((COLUMN, 8, 128), F32),
            pltpu.VMEM((2, 4, 128), F32),
            pltpu.VMEM((4, 128), F32),
            pltpu.VMEM((1, 128), F32),
            pltpu.VMEM((256, 1, 128), F32),
            pltpu.VMEM((1, 128), F32),
            pltpu.VMEM((1, 128), F32),
            pltpu.VMEM((PLANE, 1, 128), F32),
            pltpu.VMEM((DIRECT, 1, 128), F32),
            pltpu.VMEM((1, 128), F32),
            pltpu.SemaphoreType.DMA((2,)),
            pltpu.SemaphoreType.DMA,
            pltpu.SemaphoreType.DMA((2,)),
            pltpu.SemaphoreType.DMA,
            pltpu.SemaphoreType.DMA((5,)),
            pltpu.SemaphoreType.REGULAR,
        ],
        compiler_params=pltpu.CompilerParams(collective_id=0, has_side_effects=True),
        name="perambulator",
    )(source_times, spin_dilution, eig, sol)
    return pl.pallas_call(
        finish,
        out_shape=results,
        in_specs=[vmem, vmem],
        out_specs=(hbm, hbm),
        scratch_shapes=[pltpu.SemaphoreType.DMA((2,))],
        compiler_params=pltpu.CompilerParams(vmem_limit_bytes=1 << 20),
        name="finish",
    )(pltpu.with_memory_space_constraint(block, pltpu.VMEM),
      pltpu.with_memory_space_constraint(norm, pltpu.VMEM))


def solution(mesh):
    finer = Mesh(mesh.devices.reshape(NY, NXL, NXH, NZ, NC), TA + SA)
    return jax.shard_map(
        on_device,
        mesh=finer,
        in_specs=(P(None, TA, None, None, SA), P(None, TA, None, None, None, None, SA), P(), P()),
        out_specs=(P(None, TA, SA), P()),
        check_vma=False,
    )
```

```python
import functools

import jax
import jax.numpy as jnp
from jax import lax
from jax.experimental import pallas as pl
from jax.experimental.pallas import tpu as pltpu
from jax.sharding import Mesh
from jax.sharding import PartitionSpec as P

F32 = jnp.float32
BF16 = jnp.bfloat16
MESH = pl.DeviceIdType.MESH
NY, NXL, NXH, NZ, NC = 8, 2, 2, 12, 2
TA = ("y", "xl")
SA = ("xh", "z", "core")
COLUMN = NZ * NC
PLANE = NXH * NY * NXL
LATE = 13
GUESTS = 7
RELAY = 4
EARLY = (0, 1, 16, 17, 2, 3, 18, 19)
DIRECT_GUESTS = (2, 3)
OTHERS = ((4, 16), (20, 32))
FAR_Y, FAR_YS, FAR_LO = 4, 2, 10
FAR = COLUMN - FAR_LO
DIRECT = NXH * NXL * FAR_YS * FAR


def split(x):
    high = x.astype(BF16)
    low = (x - high.astype(F32)).astype(BF16)
    return high, low


def dot_rows(a, b):
    return lax.dot_general(a, b, (((1,), (1,)), ((), ())), preferred_element_type=F32)


def kernel(times_hbm, spin_hbm, eig_hbm, sol_hbm, out_ref, norm_ref,
           eig, sol, times_ref, spin_ref, high, low, tmp, send, recv, half, other,
           row, rows1, near, total, rows2, rows3, final, tally,
           sol_sem, eig_sem, int_sem, ssem, rsem, ready):
    y, xl, xh = lax.axis_index("y"), lax.axis_index("xl"), lax.axis_index("xh")
    z, core = lax.axis_index("z"), lax.axis_index("core")
    plane_me = (xh * NY + y) * NXL + xl
    place = z * NC + 1 - core
    first = plane_me == 0
    is_root = place == 0
    is_guest = jnp.logical_and(first, jnp.logical_and(place >= 1, place <= GUESTS))
    is_spare = jnp.logical_and(first, place == 1)
    is_relay = jnp.logical_and(jnp.logical_not(first), place == RELAY)
    shifted = jnp.where(place == 1, LATE, jnp.where(place <= LATE, place - 1, place))
    me = jnp.where(jnp.logical_and(first, place >= 1), shifted, place)
    in_far = jnp.logical_and(y >= FAR_Y, y < FAR_Y + FAR_YS)
    is_far = jnp.logical_and(in_far, place >= FAR_LO)
    is_early = jnp.logical_or(
        jnp.logical_and(is_root, functools.reduce(
            jnp.logical_or, [plane_me == e for e in EARLY])),
        jnp.logical_and(first, functools.reduce(
            jnp.logical_or, [place == n for n in DIRECT_GUESTS])))

    for q in range(4):
        pltpu.make_async_copy(sol_hbm.at[q % 2, q // 2], sol.at[q],
                              sol_sem.at[q // 3]).start()
    int_loads = [pltpu.make_async_copy(times_hbm, times_ref, int_sem.at[0]),
                 pltpu.make_async_copy(spin_hbm, spin_ref, int_sem.at[1])]
    for copy in int_loads:
        copy.start()

    def at_place(n):
        return {"z": n // NC, "core": 1 - lax.rem(n, NC)}

    def column(o):
        moved = jnp.where(o == LATE, 1, jnp.where(o < LATE, o + 1, o))
        return at_place(jnp.where(jnp.logical_and(first, o >= 1), moved, o))

    def plane_at(d):
        return {"xh": d // (NY * NXL), "y": d // NXL % NY, "xl": d % NXL, "z": 0, "core": 1}

    def guest(n):
        return {"xh": 0, "y": 0, "xl": 0, "z": n // NC, "core": 1 - n % NC}

    def plane(d):
        return {"xh": d // (NY * NXL), "y": lax.rem(d // NXL, NY), "xl": lax.rem(d, NXL),
                "z": 0, "core": 1}

    barrier = pltpu.get_barrier_semaphore()

    def greet(device):
        pl.semaphore_signal(barrier, inc=1, device_id=device, device_id_type=MESH)

    @pl.loop(me + 1, COLUMN)
    def _(o):
        greet(column(o))

    greet({"xh": 1 - xh})

    @pl.when(is_root)
    def _():
        @pl.loop(1, PLANE)
        def _(i):
            greet(plane(lax.rem(plane_me + i, PLANE)))

    @pl.when(is_guest)
    def _():
        @pl.loop(0, PLANE)
        def _(d):
            greet(plane(d))

    @pl.when(is_early)
    def _():
        @pl.loop(0, DIRECT)
        def _(i):
            n = FAR_LO + lax.rem(i, FAR)
            greet({"xh": i // (NXL * FAR_YS * FAR), "xl": lax.rem(i // (FAR_YS * FAR), NXL),
                   "y": FAR_Y + lax.rem(i // FAR, FAR_YS),
                   "z": n // NC, "core": 1 - lax.rem(n, NC)})

    high[...] = jnp.zeros(high.shape, BF16)
    low[...] = jnp.zeros(low.shape, BF16)

    pl.semaphore_wait(barrier, me + 1 + jnp.where(is_root, PLANE - 1 + GUESTS, 0)
                      + jnp.where(is_far, len(EARLY) + len(DIRECT_GUESTS), 0))

    @pl.loop(0, me)
    def _(o):
        pl.semaphore_signal(ready, inc=1, device_id=column(o), device_id_type=MESH)

    squares = jnp.zeros((24, 4, 512), F32)

    def arrived(buf, count, sem):
        pltpu.make_async_copy(buf.at[pl.ds(0, count)], buf.at[pl.ds(0, count)], sem).wait()

    for q in range(4):
        if q == 0:
            arrived(sol, 3, sol_sem.at[0])
        if q == 3:
            arrived(sol, 1, sol_sem.at[1])
        for c in range(3):
            piece = sol[q, :, c]
            squares = squares + piece * piece

    lanes = (squares[:, :, :128] + squares[:, :, 128:256]) + (squares[:, :, 256:384] + squares[:, :, 384:])
    sums = jnp.sum(lanes.reshape(96, 128), axis=1, keepdims=True)
    line = lax.broadcasted_iota(jnp.int32, (96, 128), 0)
    spot = lax.broadcasted_iota(jnp.int32, (96, 128), 1)
    row[...] = jnp.sum(jnp.where(line // 4 == spot, sums, F32(0)), axis=0, keepdims=True)

    def send_row(slot, sem, device):
        pltpu.make_async_remote_copy(
            src_ref=row, dst_ref=slot, send_sem=ssem, recv_sem=sem,
            device_id=device, device_id_type=MESH).start()

    @pl.when(is_far)
    def _():
        spot = ((xh * NXL + xl) * FAR_YS + y - FAR_Y) * FAR + place - FAR_LO
        send_row(rows3.at[pl.ds(spot, 1)], rsem.at[4], plane_at(EARLY[0]))
        send_row(rows1.at[pl.ds(me, 1)], rsem.at[4], {"z": 0, "core": 1})
        for n in DIRECT_GUESTS:
            send_row(rows3.at[pl.ds(spot, 1)], rsem.at[4], guest(n))
        for e in EARLY[1:]:
            send_row(rows3.at[pl.ds(spot, 1)], rsem.at[4], plane_at(e))

    @pl.when(jnp.logical_not(jnp.logical_or(is_root, is_far)))
    def _():
        send_row(rows1.at[pl.ds(me, 1)], rsem.at[0], {"z": 0, "core": 1})

    for q in range(4):
        pltpu.make_async_copy(eig_hbm.at[q % 2, q // 2], eig.at[q % 2, q // 2],
                              eig_sem).start()

    for t in range(2):
        for p in range(2):
            for c in range(3):
                h, l = split(sol[2 * t + p, :, c].reshape(96, 512))
                high[t, 128 * p:128 * p + 96, 512 * c:512 * c + 512] = h
                low[t, 128 * p:128 * p + 96, 512 * c:512 * c + 512] = l

    for copy in int_loads:
        copy.wait()
    pltpu.make_async_copy(eig, eig, eig_sem).wait()
    lane = lax.broadcasted_iota(jnp.int32, (1, 128), 1)
    lane16 = lax.broadcasted_iota(jnp.int32, (16, 128), 1)
    signs = []
    for t in range(2):
        now = (y * NXL + xl) * 2 + t
        sign = jnp.ones((1, 128), F32)
        for s in range(3):
            edge = jnp.where(now < times_ref[s], F32(-1), F32(1))
            for k in range(8):
                chir = jnp.where(spin_ref[s, k] < 2, F32(1), F32(-1))
                sign = jnp.where(lane // 4 == s * 8 + k, edge * chir, sign)
        signs.append(sign)

    for t in range(2):
        sign = signs[t]
        e = jnp.concatenate(
            [jnp.concatenate([eig[p, t, c] for c in range(3)], axis=1) for p in range(2)], axis=0)
        eh, el = split(e)
        both = dot_rows(jnp.concatenate([eh, el], axis=0), high[t])
        prod = both[:128] + (both[128:] + dot_rows(eh, low[t]))
        real = (prod[:64, :128] + prod[64:, 128:]) * sign
        imag = (prod[:64, 128:] - prod[64:, :128]) * sign
        for p, part in enumerate((real, imag)):
            tmp[:64] = part
            a0 = tmp[pl.ds(0, 16, stride=4), :]
            r1 = pltpu.roll(tmp[pl.ds(1, 16, stride=4), :], 96, 1)
            r2 = pltpu.roll(tmp[pl.ds(2, 16, stride=4), :], 64, 1)
            r3 = pltpu.roll(tmp[pl.ds(3, 16, stride=4), :], 32, 1)
            blocks = (jnp.where(lane16 < 96, a0, r1), jnp.where(lane16 < 64, r1, r2),
                      jnp.where(lane16 < 32, r2, r3))
            for r, block in enumerate(blocks):
                for h in range(2):
                    send[pl.ds(r * 8 + h * 4 + p * 2 + t, 8, stride=24), :] = block[8 * h:8 * h + 8]

    def send_block(o):
        peer = column(o)
        spot = pl.multiple_of((peer["z"] * NC + peer["core"]) * 8, 8)
        pltpu.make_async_remote_copy(
            src_ref=send.at[pl.ds(spot, 8)], dst_ref=recv.at[me],
            send_sem=ssem, recv_sem=rsem.at[1],
            device_id=peer, device_id_type=MESH).start()

    @pl.loop(0, me)
    def _(o):
        send_block(o)

    def share(source, device):
        pltpu.make_async_remote_copy(
            src_ref=source, dst_ref=rows2.at[pl.ds(plane_me, 1)], send_sem=ssem, recv_sem=rsem.at[2],
            device_id=device, device_id_type=MESH).start()

    def share_early(source):
        for e in EARLY:
            @pl.when(plane_me != e)
            def _():
                share(source, plane_at(e))

        for n in DIRECT_GUESTS:
            share(source, guest(n))

    is_far_root = jnp.logical_and(is_root, in_far)

    @pl.when(is_root)
    def _():
        rows1[0:1] = row[...]

    @pl.when(is_far_root)
    def _():
        arrived(tally, FAR_LO - 1, rsem.at[0])
        near[...] = jnp.sum(rows1[0:FAR_LO], axis=0, keepdims=True)
        share_early(near)

    @pl.when(me < COLUMN - 1)
    def _():
        pl.semaphore_wait(ready, COLUMN - 1 - me)

    @pl.loop(me + 1, COLUMN)
    def _(o):
        send_block(o)

    recv[me] = send[pl.ds(pl.multiple_of((z * NC + core) * 8, 8), 8), :]

    @pl.when(is_far_root)
    def _():
        arrived(tally, FAR, rsem.at[4])
        total[...] = near[...] + jnp.sum(rows1[FAR_LO:COLUMN], axis=0, keepdims=True)

    @pl.when(jnp.logical_and(is_root, jnp.logical_not(in_far)))
    def _():
        arrived(tally, COLUMN - 1, rsem.at[0])
        total[...] = jnp.sum(rows1[0:COLUMN], axis=0, keepdims=True)
        share_early(total)

    @pl.when(is_root)
    def _():
        for n in range(1, GUESTS + 1):
            if n not in DIRECT_GUESTS:
                share(total, guest(n))

        for low_end, high_end in OTHERS:
            @pl.loop(low_end, high_end)
            def _(d):
                @pl.when(d != plane_me)
                def _():
                    share(total, plane(d))

        rows2[pl.ds(plane_me, 1)] = total[...]

    arrived(recv, COLUMN - 1, rsem.at[1])
    block = jnp.sum(recv[...], axis=0)
    half[0] = block[:4]
    half[1] = block[4:]
    cross = pltpu.make_async_remote_copy(
        src_ref=half.at[1 - xh], dst_ref=other, send_sem=ssem, recv_sem=rsem.at[3],
        device_id={"xh": 1 - xh}, device_id_type=MESH)
    cross.start()
    cross.wait_recv()
    mine = half[xh] + other[...]
    out_ref[0] = mine[:2]
    out_ref[1] = mine[2:]

    def down(n):
        return pltpu.make_async_remote_copy(
            src_ref=final, dst_ref=final, send_sem=ssem, recv_sem=rsem.at[0],
            device_id=at_place(n), device_id_type=MESH)

    @pl.when(is_root)
    def _():
        arrived(tally, PLANE - 1, rsem.at[2])

    @pl.when(is_guest)
    def _():
        arrived(tally, PLANE, rsem.at[2])

    summing = jnp.logical_or(is_root, is_guest)

    @pl.when(summing)
    def _():
        final[...] = jnp.sum(rows2[...], axis=0, keepdims=True)

    @pl.when(is_early)
    def _():
        arrived(tally, DIRECT, rsem.at[4])
        final[...] = final[...] + jnp.sum(rows3[...], axis=0, keepdims=True)

    @pl.when(jnp.logical_not(summing))
    def _():
        down(0).wait_recv()

    plain_root = jnp.logical_and(is_root, jnp.logical_not(first))

    @pl.when(plain_root)
    def _():
        for n in range(1, RELAY + 1):
            down(n).start()

    @pl.when(is_relay)
    def _():
        @pl.loop(RELAY + 1, COLUMN)
        def _(n):
            down(n).start()

    @pl.when(is_spare)
    def _():
        @pl.loop(GUESTS + 1, COLUMN)
        def _(n):
            down(n).start()

    norm = final[...] * F32(1 / 9437184.0)
    for s in range(3):
        norm_ref[s:s + 1, :] = pltpu.roll(norm, (128 - 8 * s) % 128, 1)[:, :8]

    base = 8 * (COLUMN - 1) + 4
    roles = ((jnp.logical_and(is_root, first), PLANE - 1 + GUESTS),
             (plain_root, PLANE - 1 + GUESTS + RELAY),
             (is_relay, COLUMN - RELAY),
             (is_spare, COLUMN - GUESTS),
             (is_far, 1 + len(EARLY) + len(DIRECT_GUESTS)))
    rest = True
    for role, count in roles:
        pl.when(role)(functools.partial(arrived, tally, base + count, ssem))
        rest = jnp.logical_and(rest, jnp.logical_not(role))
    pl.when(rest)(functools.partial(arrived, tally, base + 1, ssem))


def finish(block_ref, norm_ref, block_out, norm_out, sem):
    copies = [pltpu.make_async_copy(block_ref, block_out, sem.at[0]),
              pltpu.make_async_copy(norm_ref, norm_out, sem.at[1])]
    for copy in copies:
        copy.start()
    for copy in copies:
        copy.wait()


def on_device(eigvecs, solutions, source_times, spin_dilution):
    eig = jnp.transpose(eigvecs, (0, 1, 3, 2, 4))
    sol = jnp.transpose(solutions, (0, 1, 2, 3, 5, 4, 6)).reshape(2, 2, 24, 3, 4, 512)
    vmem = pl.BlockSpec(memory_space=pltpu.VMEM)
    hbm = pl.BlockSpec(memory_space=pl.ANY)
    results = (jax.ShapeDtypeStruct((2, 2, 128), F32), jax.ShapeDtypeStruct((3, 8), F32))
    block, norm = pl.pallas_call(
        kernel,
        out_shape=(pltpu.VMEM((2, 2, 128), F32), pltpu.VMEM((3, 8), F32)),
        in_specs=[hbm, hbm, hbm, hbm],
        out_specs=(vmem, vmem),
        scratch_shapes=[
            pltpu.VMEM((2, 2, 3, 64, 512), F32),
            pltpu.VMEM((4, 24, 3, 4, 512), F32),
            pltpu.SMEM((3,), jnp.int32),
            pltpu.SMEM((3, 8), jnp.int32),
            pltpu.VMEM((2, 256, 1536), BF16),
            pltpu.VMEM((2, 256, 1536), BF16),
            pltpu.VMEM((72, 128), F32),
            pltpu.VMEM((COLUMN * 8 + 24, 128), F32),
            pltpu.VMEM((COLUMN, 8, 128), F32),
            pltpu.VMEM((2, 4, 128), F32),
            pltpu.VMEM((4, 128), F32),
            pltpu.VMEM((1, 128), F32),
            pltpu.VMEM((COLUMN, 128), F32),
            pltpu.VMEM((1, 128), F32),
            pltpu.VMEM((1, 128), F32),
            pltpu.VMEM((PLANE, 128), F32),
            pltpu.VMEM((DIRECT, 128), F32),
            pltpu.VMEM((1, 128), F32),
            pltpu.VMEM((256, 1, 128), F32),
            pltpu.SemaphoreType.DMA((2,)),
            pltpu.SemaphoreType.DMA,
            pltpu.SemaphoreType.DMA((2,)),
            pltpu.SemaphoreType.DMA,
            pltpu.SemaphoreType.DMA((5,)),
            pltpu.SemaphoreType.REGULAR,
        ],
        compiler_params=pltpu.CompilerParams(collective_id=0, has_side_effects=True),
        name="perambulator",
    )(source_times, spin_dilution, eig, sol)
    return pl.pallas_call(
        finish,
        out_shape=results,
        in_specs=[vmem, vmem],
        out_specs=(hbm, hbm),
        scratch_shapes=[pltpu.SemaphoreType.DMA((2,))],
        compiler_params=pltpu.CompilerParams(vmem_limit_bytes=1 << 20),
        name="finish",
    )(pltpu.with_memory_space_constraint(block, pltpu.VMEM),
      pltpu.with_memory_space_constraint(norm, pltpu.VMEM))


def solution(mesh):
    finer = Mesh(mesh.devices.reshape(NY, NXL, NXH, NZ, NC), TA + SA)
    return jax.shard_map(
        on_device,
        mesh=finer,
        in_specs=(P(None, TA, None, None, SA), P(None, TA, None, None, None, None, SA), P(), P()),
        out_specs=(P(None, TA, SA), P()),
        check_vma=False,
    )
```

```python
import functools

import jax
import jax.numpy as jnp
from jax import lax
from jax.experimental import pallas as pl
from jax.experimental.pallas import tpu as pltpu
from jax.sharding import Mesh
from jax.sharding import PartitionSpec as P

F32 = jnp.float32
BF16 = jnp.bfloat16
MESH = pl.DeviceIdType.MESH
NY, NXL, NXH, NZ, NC = 8, 2, 2, 12, 2
TA = ("y", "xl")
SA = ("xh", "z", "core")
COLUMN = NZ * NC
PLANE = NXH * NY * NXL
GUESTS = 7
RELAY = 4
EARLY = (0, 1, 16, 17, 2, 3, 18, 19)
DIRECT_GUESTS = (2, 3)
OTHERS = ((4, 16), (20, 32))
SLOW_LO, SLOW_HI = 3, 6
PROMPT = 16
FAR_Y, FAR_YS, FAR_LO = 4, 2, 10
FAR = COLUMN - FAR_LO
DIRECT = NXH * NXL * FAR_YS * FAR


def split(x):
    high = x.astype(BF16)
    low = (x - high.astype(F32)).astype(BF16)
    return high, low


def dot_rows(a, b):
    return lax.dot_general(a, b, (((1,), (1,)), ((), ())), preferred_element_type=F32)


def kernel(times_hbm, spin_hbm, eig_hbm, sol_hbm, out_ref, norm_ref,
           eig, sol, times_ref, spin_ref, high, low, tmp, send, recv, half, other,
           row, rows1, near, total, rows2, rows3, final, tally,
           sol_sem, eig_sem, int_sem, ssem, rsem, ready):
    y, xl, xh = lax.axis_index("y"), lax.axis_index("xl"), lax.axis_index("xh")
    z, core = lax.axis_index("z"), lax.axis_index("core")
    plane_me = (xh * NY + y) * NXL + xl
    place = z * NC + 1 - core
    first = plane_me == 0
    is_root = place == 0
    is_guest = jnp.logical_and(first, jnp.logical_and(place >= 1, place <= GUESTS))
    is_spare = jnp.logical_and(first, place == 1)
    is_relay = jnp.logical_and(jnp.logical_not(first), place == RELAY)
    me = place
    in_far = jnp.logical_and(y >= FAR_Y, y < FAR_Y + FAR_YS)
    is_far = jnp.logical_and(in_far, place >= FAR_LO)
    is_early = jnp.logical_or(
        jnp.logical_and(is_root, functools.reduce(
            jnp.logical_or, [plane_me == e for e in EARLY])),
        jnp.logical_and(first, functools.reduce(
            jnp.logical_or, [place == n for n in DIRECT_GUESTS])))

    for q in range(4):
        pltpu.make_async_copy(sol_hbm.at[q % 2, q // 2], sol.at[q],
                              sol_sem.at[q // 3]).start()
    def start_eig():
        for q in range(4):
            pltpu.make_async_copy(eig_hbm.at[q % 2, q // 2], eig.at[q % 2, q // 2],
                                  eig_sem).start()

    eager = jnp.logical_or(y < SLOW_LO, y > SLOW_HI)

    @pl.when(eager)
    def _():
        start_eig()

    int_loads = [pltpu.make_async_copy(times_hbm, times_ref, int_sem.at[0]),
                 pltpu.make_async_copy(spin_hbm, spin_ref, int_sem.at[1])]
    for copy in int_loads:
        copy.start()

    def at_place(n):
        return {"z": n // NC, "core": 1 - lax.rem(n, NC)}

    def plane_at(d):
        return {"xh": d // (NY * NXL), "y": d // NXL % NY, "xl": d % NXL, "z": 0, "core": 1}

    def guest(n):
        return {"xh": 0, "y": 0, "xl": 0, "z": n // NC, "core": 1 - n % NC}

    def plane(d):
        return {"xh": d // (NY * NXL), "y": lax.rem(d // NXL, NY), "xl": lax.rem(d, NXL),
                "z": 0, "core": 1}

    barrier = pltpu.get_barrier_semaphore()

    def greet(device):
        pl.semaphore_signal(barrier, inc=1, device_id=device, device_id_type=MESH)

    @pl.when(xh == 0)
    def _():
        greet({"xh": 1 - xh})

    @pl.loop(me + 1, COLUMN)
    def _(o):
        greet(at_place(me + COLUMN - o))

    @pl.when(is_root)
    def _():
        @pl.loop(1, PLANE)
        def _(i):
            greet(plane(lax.rem(plane_me + i, PLANE)))

    @pl.when(is_guest)
    def _():
        @pl.loop(0, PLANE)
        def _(d):
            greet(plane(d))

    @pl.when(is_early)
    def _():
        @pl.loop(0, DIRECT)
        def _(i):
            n = FAR_LO + lax.rem(i, FAR)
            greet({"xh": i // (NXL * FAR_YS * FAR), "xl": lax.rem(i // (FAR_YS * FAR), NXL),
                   "y": FAR_Y + lax.rem(i // FAR, FAR_YS),
                   "z": n // NC, "core": 1 - lax.rem(n, NC)})

    for ref in (high, low):
        for t in range(2):
            for p in range(2):
                ref[t, 128 * p + 96:128 * p + 128] = jnp.zeros((32, 1536), BF16)

    def enter():
        pl.semaphore_wait(barrier, me + xh + jnp.where(is_root, PLANE - 1 + GUESTS, 0)
                          + jnp.where(is_far, len(EARLY) + len(DIRECT_GUESTS), 0))

    def announce():
        @pl.loop(0, me)
        def _(o):
            pl.semaphore_signal(ready, inc=1, device_id=at_place(o), device_id_type=MESH)

        @pl.when(xh == 1)
        def _():
            pl.semaphore_signal(ready, inc=1, device_id={"xh": 1 - xh}, device_id_type=MESH)

    prompt = jnp.logical_and(jnp.logical_not(first), place < PROMPT)
    patient = jnp.logical_and(jnp.logical_not(first), place >= PROMPT)

    @pl.when(prompt)
    def _():
        enter()
        announce()

    squares = jnp.zeros((24, 4, 512), F32)

    def arrived(buf, count, sem):
        pltpu.make_async_copy(buf.at[pl.ds(0, count)], buf.at[pl.ds(0, count)], sem).wait()

    for q in range(4):
        if q == 0:
            arrived(sol, 3, sol_sem.at[0])
        if q == 3:
            arrived(sol, 1, sol_sem.at[1])
        for c in range(3):
            piece = sol[q, :, c]
            squares = squares + piece * piece

    lanes = (squares[:, :, :128] + squares[:, :, 128:256]) + (squares[:, :, 256:384] + squares[:, :, 384:])
    sums = jnp.sum(lanes.reshape(96, 128), axis=1, keepdims=True)
    line = lax.broadcasted_iota(jnp.int32, (96, 128), 0)
    spot = lax.broadcasted_iota(jnp.int32, (96, 128), 1)
    row[...] = jnp.sum(jnp.where(line // 4 == spot, sums, F32(0)), axis=0, keepdims=True)

    def send_row(slot, sem, device):
        pltpu.make_async_remote_copy(
            src_ref=row, dst_ref=slot, send_sem=ssem, recv_sem=sem,
            device_id=device, device_id_type=MESH).start()

    @pl.when(patient)
    def _():
        enter()

    @pl.when(is_far)
    def _():
        spot = ((xh * NXL + xl) * FAR_YS + y - FAR_Y) * FAR + place - FAR_LO
        send_row(rows3.at[pl.ds(spot, 1)], rsem.at[4], plane_at(EARLY[0]))
        send_row(rows1.at[pl.ds(me, 1)], rsem.at[4], {"z": 0, "core": 1})
        for n in DIRECT_GUESTS:
            send_row(rows3.at[pl.ds(spot, 1)], rsem.at[4], guest(n))
        for e in EARLY[1:]:
            send_row(rows3.at[pl.ds(spot, 1)], rsem.at[4], plane_at(e))

    @pl.when(jnp.logical_not(functools.reduce(jnp.logical_or, [is_root, is_far, first])))
    def _():
        send_row(rows1.at[pl.ds(me, 1)], rsem.at[0], {"z": 0, "core": 1})

    @pl.when(patient)
    def _():
        announce()

    @pl.when(jnp.logical_not(eager))
    def _():
        start_eig()

    for t in range(2):
        for p in range(2):
            for c in range(3):
                h, l = split(sol[2 * t + p, :, c].reshape(96, 512))
                high[t, 128 * p:128 * p + 96, 512 * c:512 * c + 512] = h
                low[t, 128 * p:128 * p + 96, 512 * c:512 * c + 512] = l

    for copy in int_loads:
        copy.wait()
    pltpu.make_async_copy(eig, eig, eig_sem).wait()
    lane = lax.broadcasted_iota(jnp.int32, (1, 128), 1)
    lane16 = lax.broadcasted_iota(jnp.int32, (16, 128), 1)
    signs = []
    for t in range(2):
        now = (y * NXL + xl) * 2 + t
        sign = jnp.ones((1, 128), F32)
        for s in range(3):
            edge = jnp.where(now < times_ref[s], F32(-1), F32(1))
            for k in range(8):
                chir = jnp.where(spin_ref[s, k] < 2, F32(1), F32(-1))
                sign = jnp.where(lane // 4 == s * 8 + k, edge * chir, sign)
        signs.append(sign)

    for t in range(2):
        sign = signs[t]
        e = jnp.concatenate(
            [jnp.concatenate([eig[p, t, c] for c in range(3)], axis=1) for p in range(2)], axis=0)
        eh, el = split(e)
        both = dot_rows(jnp.concatenate([eh, el], axis=0), high[t])
        prod = both[:128] + (both[128:] + dot_rows(eh, low[t]))
        real = (prod[:64, :128] + prod[64:, 128:]) * sign
        imag = (prod[:64, 128:] - prod[64:, :128]) * sign
        for p, part in enumerate((real, imag)):
            tmp[:64] = part
            a0 = tmp[pl.ds(0, 16, stride=4), :]
            r1 = pltpu.roll(tmp[pl.ds(1, 16, stride=4), :], 96, 1)
            r2 = pltpu.roll(tmp[pl.ds(2, 16, stride=4), :], 64, 1)
            r3 = pltpu.roll(tmp[pl.ds(3, 16, stride=4), :], 32, 1)
            blocks = (jnp.where(lane16 < 96, a0, r1), jnp.where(lane16 < 64, r1, r2),
                      jnp.where(lane16 < 32, r2, r3))
            for r, block in enumerate(blocks):
                for h in range(2):
                    send[pl.ds(r * 8 + h * 4 + p * 2 + t, 8, stride=24), :] = block[8 * h:8 * h + 8]

    @pl.when(first)
    def _():
        enter()

        @pl.when(jnp.logical_not(is_root))
        def _():
            announce()
            send_row(rows1.at[pl.ds(me, 1)], rsem.at[0], {"z": 0, "core": 1})

    def send_block(o):
        peer = at_place(o)
        spot = pl.multiple_of((peer["z"] * NC + peer["core"]) * 8, 8)
        pltpu.make_async_remote_copy(
            src_ref=send.at[pl.ds(spot, 8)], dst_ref=recv.at[me],
            send_sem=ssem, recv_sem=rsem.at[1],
            device_id=peer, device_id_type=MESH).start()

    @pl.loop(0, me)
    def _(o):
        send_block(o)

    def share(source, device):
        pltpu.make_async_remote_copy(
            src_ref=source, dst_ref=rows2.at[pl.ds(plane_me, 1)], send_sem=ssem, recv_sem=rsem.at[2],
            device_id=device, device_id_type=MESH).start()

    def share_early(source):
        for e in EARLY:
            @pl.when(plane_me != e)
            def _():
                share(source, plane_at(e))

        for n in DIRECT_GUESTS:
            share(source, guest(n))

    is_far_root = jnp.logical_and(is_root, in_far)

    @pl.when(is_root)
    def _():
        rows1[0:1] = row[...]

    @pl.when(is_far_root)
    def _():
        arrived(tally, FAR_LO - 1, rsem.at[0])
        near[...] = jnp.sum(rows1[0:FAR_LO], axis=0, keepdims=True)
        share_early(near)

    @pl.when(jnp.logical_or(me < COLUMN - 1, xh == 0))
    def _():
        pl.semaphore_wait(ready, COLUMN - me - xh)

    @pl.loop(me + 1, COLUMN)
    def _(o):
        send_block(o)

    recv[me] = send[pl.ds(pl.multiple_of((z * NC + core) * 8, 8), 8), :]

    @pl.when(is_far_root)
    def _():
        arrived(tally, FAR, rsem.at[4])
        total[...] = near[...] + jnp.sum(rows1[FAR_LO:COLUMN], axis=0, keepdims=True)

    @pl.when(jnp.logical_and(is_root, jnp.logical_not(in_far)))
    def _():
        arrived(tally, COLUMN - 1, rsem.at[0])
        total[...] = jnp.sum(rows1[0:COLUMN], axis=0, keepdims=True)
        share_early(total)

    @pl.when(is_root)
    def _():
        for n in range(1, GUESTS + 1):
            if n not in DIRECT_GUESTS:
                share(total, guest(n))

        for low_end, high_end in OTHERS:
            @pl.loop(low_end, high_end)
            def _(d):
                @pl.when(d != plane_me)
                def _():
                    share(total, plane(d))

        rows2[pl.ds(plane_me, 1)] = total[...]

    arrived(recv, COLUMN - 1, rsem.at[1])
    block = jnp.sum(recv[...], axis=0)
    half[0] = block[:4]
    half[1] = block[4:]
    cross = pltpu.make_async_remote_copy(
        src_ref=half.at[1 - xh], dst_ref=other, send_sem=ssem, recv_sem=rsem.at[3],
        device_id={"xh": 1 - xh}, device_id_type=MESH)
    cross.start()
    cross.wait_recv()
    mine = half[xh] + other[...]
    out_ref[0] = mine[:2]
    out_ref[1] = mine[2:]

    def down(n):
        return pltpu.make_async_remote_copy(
            src_ref=final, dst_ref=final, send_sem=ssem, recv_sem=rsem.at[0],
            device_id=at_place(n), device_id_type=MESH)

    @pl.when(is_root)
    def _():
        arrived(tally, PLANE - 1, rsem.at[2])

    @pl.when(is_guest)
    def _():
        arrived(tally, PLANE, rsem.at[2])

    summing = jnp.logical_or(is_root, is_guest)

    @pl.when(summing)
    def _():
        final[...] = jnp.sum(rows2[...], axis=0, keepdims=True)

    @pl.when(is_early)
    def _():
        arrived(tally, DIRECT, rsem.at[4])
        final[...] = final[...] + jnp.sum(rows3[...], axis=0, keepdims=True)

    @pl.when(jnp.logical_not(summing))
    def _():
        down(0).wait_recv()

    plain_root = jnp.logical_and(is_root, jnp.logical_not(first))

    @pl.when(plain_root)
    def _():
        for n in range(1, RELAY + 1):
            down(n).start()

    @pl.when(is_relay)
    def _():
        @pl.loop(RELAY + 1, COLUMN)
        def _(n):
            down(n).start()

    @pl.when(is_spare)
    def _():
        @pl.loop(GUESTS + 1, COLUMN)
        def _(n):
            down(n).start()

    norm = final[...] * F32(1 / 9437184.0)
    for s in range(3):
        norm_ref[s:s + 1, :] = pltpu.roll(norm, (128 - 8 * s) % 128, 1)[:, :8]

    base = 8 * (COLUMN - 1) + 4
    roles = ((jnp.logical_and(is_root, first), PLANE - 1 + GUESTS),
             (plain_root, PLANE - 1 + GUESTS + RELAY),
             (is_relay, COLUMN - RELAY),
             (is_spare, COLUMN - GUESTS),
             (is_far, 1 + len(EARLY) + len(DIRECT_GUESTS)))
    rest = True
    for role, count in roles:
        pl.when(role)(functools.partial(arrived, tally, base + count, ssem))
        rest = jnp.logical_and(rest, jnp.logical_not(role))
    pl.when(rest)(functools.partial(arrived, tally, base + 1, ssem))


def finish(block_ref, norm_ref, block_out, norm_out, sem):
    copies = [pltpu.make_async_copy(block_ref, block_out, sem.at[0]),
              pltpu.make_async_copy(norm_ref, norm_out, sem.at[1])]
    for copy in copies:
        copy.start()
    for copy in copies:
        copy.wait()


def on_device(eigvecs, solutions, source_times, spin_dilution):
    eig = jnp.transpose(eigvecs, (0, 1, 3, 2, 4))
    sol = jnp.transpose(solutions, (0, 1, 2, 3, 5, 4, 6)).reshape(2, 2, 24, 3, 4, 512)
    vmem = pl.BlockSpec(memory_space=pltpu.VMEM)
    hbm = pl.BlockSpec(memory_space=pl.ANY)
    results = (jax.ShapeDtypeStruct((2, 2, 128), F32), jax.ShapeDtypeStruct((3, 8), F32))
    block, norm = pl.pallas_call(
        kernel,
        out_shape=(pltpu.VMEM((2, 2, 128), F32), pltpu.VMEM((3, 8), F32)),
        in_specs=[hbm, hbm, hbm, hbm],
        out_specs=(vmem, vmem),
        scratch_shapes=[
            pltpu.VMEM((2, 2, 3, 64, 512), F32),
            pltpu.VMEM((4, 24, 3, 4, 512), F32),
            pltpu.SMEM((3,), jnp.int32),
            pltpu.SMEM((3, 8), jnp.int32),
            pltpu.VMEM((2, 256, 1536), BF16),
            pltpu.VMEM((2, 256, 1536), BF16),
            pltpu.VMEM((72, 128), F32),
            pltpu.VMEM((COLUMN * 8 + 24, 128), F32),
            pltpu.VMEM((COLUMN, 8, 128), F32),
            pltpu.VMEM((2, 4, 128), F32),
            pltpu.VMEM((4, 128), F32),
            pltpu.VMEM((1, 128), F32),
            pltpu.VMEM((COLUMN, 128), F32),
            pltpu.VMEM((1, 128), F32),
            pltpu.VMEM((1, 128), F32),
            pltpu.VMEM((PLANE, 128), F32),
            pltpu.VMEM((DIRECT, 128), F32),
            pltpu.VMEM((1, 128), F32),
            pltpu.VMEM((256, 1, 128), F32),
            pltpu.SemaphoreType.DMA((2,)),
            pltpu.SemaphoreType.DMA,
            pltpu.SemaphoreType.DMA((2,)),
            pltpu.SemaphoreType.DMA,
            pltpu.SemaphoreType.DMA((5,)),
            pltpu.SemaphoreType.REGULAR,
        ],
        compiler_params=pltpu.CompilerParams(collective_id=0, has_side_effects=True),
        name="perambulator",
    )(source_times, spin_dilution, eig, sol)
    return pl.pallas_call(
        finish,
        out_shape=results,
        in_specs=[vmem, vmem],
        out_specs=(hbm, hbm),
        scratch_shapes=[pltpu.SemaphoreType.DMA((2,))],
        compiler_params=pltpu.CompilerParams(vmem_limit_bytes=1 << 20),
        name="finish",
    )(pltpu.with_memory_space_constraint(block, pltpu.VMEM),
      pltpu.with_memory_space_constraint(norm, pltpu.VMEM))


def solution(mesh):
    finer = Mesh(mesh.devices.reshape(NY, NXL, NXH, NZ, NC), TA + SA)
    return jax.shard_map(
        on_device,
        mesh=finer,
        in_specs=(P(None, TA, None, None, SA), P(None, TA, None, None, None, None, SA), P(), P()),
        out_specs=(P(None, TA, SA), P()),
        check_vma=False,
    )
```

```python
import functools

import jax
import jax.numpy as jnp
from jax import lax
from jax.experimental import pallas as pl
from jax.experimental.pallas import tpu as pltpu
from jax.sharding import Mesh
from jax.sharding import PartitionSpec as P

F32 = jnp.float32
BF16 = jnp.bfloat16
MESH = pl.DeviceIdType.MESH
NY, NXL, NXH, NZ, NC = 8, 2, 2, 12, 2
TA = ("y", "xl")
SA = ("xh", "z", "core")
COLUMN = NZ * NC
PLANE = NXH * NY * NXL
GUESTS = 7
RELAY = 4
EARLY = (0, 1, 16, 17, 2, 3, 18, 19)
DIRECT_GUESTS = (2, 3)
OTHERS = ((4, 16), (20, 32))
SLOW_LO, SLOW_HI = 3, 6
PROMPT = 16
CUT = 18
FAR_Y, FAR_YS, FAR_LO = 4, 2, 10
FAR = COLUMN - FAR_LO
DIRECT = NXH * NXL * FAR_YS * FAR


def split(x):
    high = x.astype(BF16)
    low = (x - high.astype(F32)).astype(BF16)
    return high, low


def dot_rows(a, b):
    return lax.dot_general(a, b, (((1,), (1,)), ((), ())), preferred_element_type=F32)


def kernel(times_hbm, spin_hbm, eig_hbm, sol_hbm, out_ref, norm_ref,
           eig, sol, times_ref, spin_ref, high, low, tmp, send, recv, half, other,
           row, rows1, near, total, rows2, rows3, final, tally,
           loads, ssem, rsem, ready):
    y, xl, xh = lax.axis_index("y"), lax.axis_index("xl"), lax.axis_index("xh")
    z, core = lax.axis_index("z"), lax.axis_index("core")
    plane_me = (xh * NY + y) * NXL + xl
    place = z * NC + 1 - core
    first = plane_me == 0
    is_root = place == 0
    is_guest = jnp.logical_and(first, jnp.logical_and(place >= 1, place <= GUESTS))
    is_spare = jnp.logical_and(first, place == 1)
    is_relay = jnp.logical_and(jnp.logical_not(first), place == RELAY)
    me = place
    in_far = jnp.logical_and(y >= FAR_Y, y < FAR_Y + FAR_YS)
    is_far = jnp.logical_and(in_far, place >= FAR_LO)
    is_early = jnp.logical_or(
        jnp.logical_and(is_root, functools.reduce(
            jnp.logical_or, [plane_me == e for e in EARLY])),
        jnp.logical_and(first, functools.reduce(
            jnp.logical_or, [place == n for n in DIRECT_GUESTS])))

    for q in range(3):
        pltpu.make_async_copy(sol_hbm.at[q % 2, q // 2], sol.at[pl.ds(24 * q, 24)],
                              loads.at[0]).start()
    pltpu.make_async_copy(sol_hbm.at[1, 1, pl.ds(0, CUT)], sol.at[pl.ds(72, CUT)],
                          loads.at[1]).start()
    pltpu.make_async_copy(sol_hbm.at[1, 1, pl.ds(CUT, 24 - CUT)],
                          sol.at[pl.ds(72 + CUT, 24 - CUT)], loads.at[2]).start()

    def start_eig():
        for q in range(4):
            pltpu.make_async_copy(eig_hbm.at[q % 2, q // 2], eig.at[q % 2, q // 2],
                                  loads.at[0]).start()

    eager = jnp.logical_or(y < SLOW_LO, y > SLOW_HI)
    int_loads = [pltpu.make_async_copy(times_hbm, times_ref, loads.at[1]),
                 pltpu.make_async_copy(spin_hbm, spin_ref, loads.at[2])]

    def at_place(n):
        return {"z": n // NC, "core": 1 - lax.rem(n, NC)}

    def plane_at(d):
        return {"xh": d // (NY * NXL), "y": d // NXL % NY, "xl": d % NXL, "z": 0, "core": 1}

    def guest(n):
        return {"xh": 0, "y": 0, "xl": 0, "z": n // NC, "core": 1 - n % NC}

    def plane(d):
        return {"xh": d // (NY * NXL), "y": lax.rem(d // NXL, NY), "xl": lax.rem(d, NXL),
                "z": 0, "core": 1}

    barrier = pltpu.get_barrier_semaphore()

    def greet(device):
        pl.semaphore_signal(barrier, inc=1, device_id=device, device_id_type=MESH)

    @pl.when(xh == 0)
    def _():
        greet({"xh": 1 - xh})

    @pl.loop(me + 1, COLUMN)
    def _(o):
        greet(at_place(me + COLUMN - o))

    @pl.when(is_root)
    def _():
        @pl.loop(1, PLANE)
        def _(i):
            greet(plane(lax.rem(plane_me + i, PLANE)))

    @pl.when(is_guest)
    def _():
        @pl.loop(0, PLANE)
        def _(d):
            greet(plane(d))

    @pl.when(is_early)
    def _():
        @pl.loop(0, DIRECT)
        def _(i):
            n = FAR_LO + lax.rem(i, FAR)
            greet({"xh": i // (NXL * FAR_YS * FAR), "xl": lax.rem(i // (FAR_YS * FAR), NXL),
                   "y": FAR_Y + lax.rem(i // FAR, FAR_YS),
                   "z": n // NC, "core": 1 - lax.rem(n, NC)})

    for ref in (high, low):
        for t in range(2):
            for p in range(2):
                ref[t, 128 * p + 96:128 * p + 128] = jnp.zeros((32, 1536), BF16)

    def enter():
        pl.semaphore_wait(barrier, me + xh + jnp.where(is_root, PLANE - 1 + GUESTS, 0)
                          + jnp.where(is_far, len(EARLY) + len(DIRECT_GUESTS), 0))

    def announce():
        @pl.loop(0, me)
        def _(o):
            pl.semaphore_signal(ready, inc=1, device_id=at_place(o), device_id_type=MESH)

        @pl.when(xh == 1)
        def _():
            pl.semaphore_signal(ready, inc=1, device_id={"xh": 1 - xh}, device_id_type=MESH)

    prompt = jnp.logical_and(jnp.logical_not(first), place < PROMPT)
    patient = jnp.logical_and(jnp.logical_not(first), place >= PROMPT)

    @pl.when(prompt)
    def _():
        enter()
        announce()

    def arrived(buf, count, sem):
        pltpu.make_async_copy(buf.at[pl.ds(0, count)], buf.at[pl.ds(0, count)], sem).wait()

    def squared(acc, start, count):
        for c in range(3):
            piece = sol[start:start + count, c]
            acc = acc + piece * piece
        return acc

    def as_row(acc, start, count):
        lanes = (acc[:, :, :128] + acc[:, :, 128:256]) + (acc[:, :, 256:384] + acc[:, :, 384:])
        sums = jnp.sum(lanes.reshape(count * 4, 128), axis=1, keepdims=True)
        line = lax.broadcasted_iota(jnp.int32, (count * 4, 128), 0)
        spot = lax.broadcasted_iota(jnp.int32, (count * 4, 128), 1)
        return jnp.sum(jnp.where(line // 4 + start == spot, sums, F32(0)), axis=0, keepdims=True)

    squares = jnp.zeros((CUT, 4, 512), F32)
    more = jnp.zeros((24 - CUT, 4, 512), F32)
    arrived(sol, 72, loads.at[0])

    @pl.when(eager)
    def _():
        start_eig()

    for q in range(3):
        squares = squared(squares, 24 * q, CUT)
        more = squared(more, 24 * q + CUT, 24 - CUT)
    arrived(sol, CUT, loads.at[1])
    part = as_row(squared(squares, 72, CUT), 0, CUT)
    arrived(sol, 24 - CUT, loads.at[2])
    row[...] = part + as_row(squared(more, 72 + CUT, 24 - CUT), CUT, 24 - CUT)

    def send_row(slot, sem, device):
        pltpu.make_async_remote_copy(
            src_ref=row, dst_ref=slot, send_sem=ssem, recv_sem=sem,
            device_id=device, device_id_type=MESH).start()

    @pl.when(patient)
    def _():
        enter()

    @pl.when(is_far)
    def _():
        spot = ((xh * NXL + xl) * FAR_YS + y - FAR_Y) * FAR + place - FAR_LO
        send_row(rows3.at[pl.ds(spot, 1)], rsem.at[4], plane_at(EARLY[0]))
        send_row(rows1.at[pl.ds(me, 1)], rsem.at[4], {"z": 0, "core": 1})
        for n in DIRECT_GUESTS:
            send_row(rows3.at[pl.ds(spot, 1)], rsem.at[4], guest(n))
        for e in EARLY[1:]:
            send_row(rows3.at[pl.ds(spot, 1)], rsem.at[4], plane_at(e))

    @pl.when(jnp.logical_not(functools.reduce(jnp.logical_or, [is_root, is_far, first])))
    def _():
        send_row(rows1.at[pl.ds(me, 1)], rsem.at[0], {"z": 0, "core": 1})

    @pl.when(patient)
    def _():
        announce()

    @pl.when(jnp.logical_not(eager))
    def _():
        start_eig()

    for copy in int_loads:
        copy.start()

    for t in range(2):
        for p in range(2):
            for c in range(3):
                q = 2 * t + p
                h, l = split(sol[24 * q:24 * q + 24, c].reshape(96, 512))
                high[t, 128 * p:128 * p + 96, 512 * c:512 * c + 512] = h
                low[t, 128 * p:128 * p + 96, 512 * c:512 * c + 512] = l

    for copy in int_loads:
        copy.wait()
    pltpu.make_async_copy(eig, eig, loads.at[0]).wait()
    lane = lax.broadcasted_iota(jnp.int32, (1, 128), 1)
    lane16 = lax.broadcasted_iota(jnp.int32, (16, 128), 1)
    signs = []
    for t in range(2):
        now = (y * NXL + xl) * 2 + t
        sign = jnp.ones((1, 128), F32)
        for s in range(3):
            edge = jnp.where(now < times_ref[s], F32(-1), F32(1))
            for k in range(8):
                chir = jnp.where(spin_ref[s, k] < 2, F32(1), F32(-1))
                sign = jnp.where(lane // 4 == s * 8 + k, edge * chir, sign)
        signs.append(sign)

    for t in range(2):
        sign = signs[t]
        e = jnp.concatenate(
            [jnp.concatenate([eig[p, t, c] for c in range(3)], axis=1) for p in range(2)], axis=0)
        eh, el = split(e)
        both = dot_rows(jnp.concatenate([eh, el], axis=0), high[t])
        prod = both[:128] + (both[128:] + dot_rows(eh, low[t]))
        real = (prod[:64, :128] + prod[64:, 128:]) * sign
        imag = (prod[:64, 128:] - prod[64:, :128]) * sign
        for p, part in enumerate((real, imag)):
            tmp[:64] = part
            a0 = tmp[pl.ds(0, 16, stride=4), :]
            r1 = pltpu.roll(tmp[pl.ds(1, 16, stride=4), :], 96, 1)
            r2 = pltpu.roll(tmp[pl.ds(2, 16, stride=4), :], 64, 1)
            r3 = pltpu.roll(tmp[pl.ds(3, 16, stride=4), :], 32, 1)
            blocks = (jnp.where(lane16 < 96, a0, r1), jnp.where(lane16 < 64, r1, r2),
                      jnp.where(lane16 < 32, r2, r3))
            for r, block in enumerate(blocks):
                for h in range(2):
                    send[pl.ds(r * 8 + h * 4 + p * 2 + t, 8, stride=24), :] = block[8 * h:8 * h + 8]

    @pl.when(first)
    def _():
        enter()

        @pl.when(jnp.logical_not(is_root))
        def _():
            announce()
            send_row(rows1.at[pl.ds(me, 1)], rsem.at[0], {"z": 0, "core": 1})

    def send_block(o):
        peer = at_place(o)
        spot = pl.multiple_of((peer["z"] * NC + peer["core"]) * 8, 8)
        pltpu.make_async_remote_copy(
            src_ref=send.at[pl.ds(spot, 8)], dst_ref=recv.at[me],
            send_sem=ssem, recv_sem=rsem.at[1],
            device_id=peer, device_id_type=MESH).start()

    @pl.loop(0, me)
    def _(o):
        send_block(o)

    def share(source, device):
        pltpu.make_async_remote_copy(
            src_ref=source, dst_ref=rows2.at[pl.ds(plane_me, 1)], send_sem=ssem, recv_sem=rsem.at[2],
            device_id=device, device_id_type=MESH).start()

    def share_early(source):
        for e in EARLY:
            @pl.when(plane_me != e)
            def _():
                share(source, plane_at(e))

        for n in DIRECT_GUESTS:
            share(source, guest(n))

    is_far_root = jnp.logical_and(is_root, in_far)

    @pl.when(is_root)
    def _():
        rows1[0:1] = row[...]

    @pl.when(is_far_root)
    def _():
        arrived(tally, FAR_LO - 1, rsem.at[0])
        near[...] = jnp.sum(rows1[0:FAR_LO], axis=0, keepdims=True)
        share_early(near)

    @pl.when(jnp.logical_or(me < COLUMN - 1, xh == 0))
    def _():
        pl.semaphore_wait(ready, COLUMN - me - xh)

    @pl.loop(me + 1, COLUMN)
    def _(o):
        send_block(o)

    recv[me] = send[pl.ds(pl.multiple_of((z * NC + core) * 8, 8), 8), :]

    @pl.when(is_far_root)
    def _():
        arrived(tally, FAR, rsem.at[4])
        total[...] = near[...] + jnp.sum(rows1[FAR_LO:COLUMN], axis=0, keepdims=True)

    @pl.when(jnp.logical_and(is_root, jnp.logical_not(in_far)))
    def _():
        arrived(tally, COLUMN - 1, rsem.at[0])
        total[...] = jnp.sum(rows1[0:COLUMN], axis=0, keepdims=True)
        share_early(total)

    @pl.when(is_root)
    def _():
        for n in range(1, GUESTS + 1):
            if n not in DIRECT_GUESTS:
                share(total, guest(n))

        for low_end, high_end in OTHERS:
            @pl.loop(low_end, high_end)
            def _(d):
                @pl.when(d != plane_me)
                def _():
                    share(total, plane(d))

        rows2[pl.ds(plane_me, 1)] = total[...]

    arrived(recv, COLUMN - 1, rsem.at[1])
    block = jnp.sum(recv[...], axis=0)
    half[0] = block[:4]
    half[1] = block[4:]
    cross = pltpu.make_async_remote_copy(
        src_ref=half.at[1 - xh], dst_ref=other, send_sem=ssem, recv_sem=rsem.at[3],
        device_id={"xh": 1 - xh}, device_id_type=MESH)
    cross.start()
    cross.wait_recv()
    mine = half[xh] + other[...]
    out_ref[0] = mine[:2]
    out_ref[1] = mine[2:]

    def down(n):
        return pltpu.make_async_remote_copy(
            src_ref=final, dst_ref=final, send_sem=ssem, recv_sem=rsem.at[0],
            device_id=at_place(n), device_id_type=MESH)

    base = 8 * (COLUMN - 1) + 4
    plain_root = jnp.logical_and(is_root, jnp.logical_not(first))
    first_root = jnp.logical_and(is_root, first)
    senders = ((plain_root, PLANE - 1 + GUESTS + RELAY),
               (is_relay, COLUMN - RELAY),
               (is_spare, COLUMN - GUESTS))
    others = jnp.logical_not(functools.reduce(
        jnp.logical_or, [plain_root, is_relay, is_spare, first_root, is_far]))
    for role, count in ((first_root, PLANE - 1 + GUESTS),
                        (is_far, 1 + len(EARLY) + len(DIRECT_GUESTS)), (others, 1)):
        pl.when(role)(functools.partial(arrived, tally, base + count, ssem))

    @pl.when(is_root)
    def _():
        arrived(tally, PLANE - 1, rsem.at[2])

    @pl.when(is_guest)
    def _():
        arrived(tally, PLANE, rsem.at[2])

    summing = jnp.logical_or(is_root, is_guest)

    @pl.when(summing)
    def _():
        final[...] = jnp.sum(rows2[...], axis=0, keepdims=True)

    @pl.when(is_early)
    def _():
        arrived(tally, DIRECT, rsem.at[4])
        final[...] = final[...] + jnp.sum(rows3[...], axis=0, keepdims=True)

    @pl.when(jnp.logical_not(summing))
    def _():
        down(0).wait_recv()

    @pl.when(plain_root)
    def _():
        for n in range(1, RELAY + 1):
            down(n).start()

    @pl.when(is_relay)
    def _():
        @pl.loop(RELAY + 1, COLUMN)
        def _(n):
            down(n).start()

    @pl.when(is_spare)
    def _():
        @pl.loop(GUESTS + 1, COLUMN)
        def _(n):
            down(n).start()

    norm = final[...] * F32(1 / 9437184.0)
    for s in range(3):
        norm_ref[s:s + 1, :] = pltpu.roll(norm, (128 - 8 * s) % 128, 1)[:, :8]

    for role, count in senders:
        pl.when(role)(functools.partial(arrived, tally, base + count, ssem))


def finish(block_ref, norm_ref, block_out, norm_out, sem):
    copies = [pltpu.make_async_copy(block_ref, block_out, sem.at[0]),
              pltpu.make_async_copy(norm_ref, norm_out, sem.at[1])]
    for copy in copies:
        copy.start()
    for copy in copies:
        copy.wait()


def on_device(eigvecs, solutions, source_times, spin_dilution):
    eig = jnp.transpose(eigvecs, (0, 1, 3, 2, 4))
    sol = jnp.transpose(solutions, (0, 1, 2, 3, 5, 4, 6)).reshape(2, 2, 24, 3, 4, 512)
    vmem = pl.BlockSpec(memory_space=pltpu.VMEM)
    hbm = pl.BlockSpec(memory_space=pl.ANY)
    results = (jax.ShapeDtypeStruct((2, 2, 128), F32), jax.ShapeDtypeStruct((3, 8), F32))
    block, norm = pl.pallas_call(
        kernel,
        out_shape=(pltpu.VMEM((2, 2, 128), F32), pltpu.VMEM((3, 8), F32)),
        in_specs=[hbm, hbm, hbm, hbm],
        out_specs=(vmem, vmem),
        scratch_shapes=[
            pltpu.VMEM((2, 2, 3, 64, 512), F32),
            pltpu.VMEM((96, 3, 4, 512), F32),
            pltpu.SMEM((3,), jnp.int32),
            pltpu.SMEM((3, 8), jnp.int32),
            pltpu.VMEM((2, 256, 1536), BF16),
            pltpu.VMEM((2, 256, 1536), BF16),
            pltpu.VMEM((72, 128), F32),
            pltpu.VMEM((COLUMN * 8 + 24, 128), F32),
            pltpu.VMEM((COLUMN, 8, 128), F32),
            pltpu.VMEM((2, 4, 128), F32),
            pltpu.VMEM((4, 128), F32),
            pltpu.VMEM((1, 128), F32),
            pltpu.VMEM((COLUMN, 128), F32),
            pltpu.VMEM((1, 128), F32),
            pltpu.VMEM((1, 128), F32),
            pltpu.VMEM((PLANE, 128), F32),
            pltpu.VMEM((DIRECT, 128), F32),
            pltpu.VMEM((1, 128), F32),
            pltpu.VMEM((256, 1, 128), F32),
            pltpu.SemaphoreType.DMA((3,)),
            pltpu.SemaphoreType.DMA,
            pltpu.SemaphoreType.DMA((5,)),
            pltpu.SemaphoreType.REGULAR,
        ],
        compiler_params=pltpu.CompilerParams(collective_id=0, has_side_effects=True),
        name="perambulator",
    )(source_times, spin_dilution, eig, sol)
    return pl.pallas_call(
        finish,
        out_shape=results,
        in_specs=[vmem, vmem],
        out_specs=(hbm, hbm),
        scratch_shapes=[pltpu.SemaphoreType.DMA((2,))],
        compiler_params=pltpu.CompilerParams(vmem_limit_bytes=1 << 20),
        name="finish",
    )(pltpu.with_memory_space_constraint(block, pltpu.VMEM),
      pltpu.with_memory_space_constraint(norm, pltpu.VMEM))


def solution(mesh):
    finer = Mesh(mesh.devices.reshape(NY, NXL, NXH, NZ, NC), TA + SA)
    return jax.shard_map(
        on_device,
        mesh=finer,
        in_specs=(P(None, TA, None, None, SA), P(None, TA, None, None, None, None, SA), P(), P()),
        out_specs=(P(None, TA, SA), P()),
        check_vma=False,
    )
```

```python
import functools

import jax
import jax.numpy as jnp
from jax import lax
from jax.experimental import pallas as pl
from jax.experimental.pallas import tpu as pltpu
from jax.sharding import Mesh
from jax.sharding import PartitionSpec as P

F32 = jnp.float32
BF16 = jnp.bfloat16
MESH = pl.DeviceIdType.MESH
NY, NXL, NXH, NZ, NC = 8, 2, 2, 12, 2
TA = ("y", "xl")
SA = ("xh", "z", "core")
COLUMN = NZ * NC
PLANE = NXH * NY * NXL
GUESTS = 7
RELAY = 4
EARLY = (0, 1, 16, 17, 2, 3, 18, 19)
DIRECT_GUESTS = (2, 3)
OTHERS = ((4, 16), (20, 32))
SLOW_LO, SLOW_HI = 3, 6
PROMPT = 16
FAR_Y, FAR_YS, FAR_LO = 4, 2, 12
FAR = COLUMN - FAR_LO
DIRECT = NXH * NXL * FAR_YS * FAR


def split(x):
    high = x.astype(BF16)
    low = (x - high.astype(F32)).astype(BF16)
    return high, low


def dot_rows(a, b):
    return lax.dot_general(a, b, (((1,), (1,)), ((), ())), preferred_element_type=F32)


def kernel(times_hbm, spin_hbm, eig_hbm, sol_hbm, out_ref, norm_ref,
           eig, sol, times_ref, spin_ref, high, low, tmp, send, recv, half, other,
           row, rows1, near, total, rows2, rows3, final, tally,
           sol_sem, eig_sem, int_sem, ssem, rsem, ready):
    y, xl, xh = lax.axis_index("y"), lax.axis_index("xl"), lax.axis_index("xh")
    z, core = lax.axis_index("z"), lax.axis_index("core")
    plane_me = (xh * NY + y) * NXL + xl
    place = z * NC + 1 - core
    first = plane_me == 0
    is_root = place == 0
    is_guest = jnp.logical_and(first, jnp.logical_and(place >= 1, place <= GUESTS))
    is_spare = jnp.logical_and(first, place == 1)
    is_relay = jnp.logical_and(jnp.logical_not(first), place == RELAY)
    me = place
    in_far = jnp.logical_and(y >= FAR_Y, y < FAR_Y + FAR_YS)
    is_far = jnp.logical_and(in_far, place >= FAR_LO)
    is_early = jnp.logical_or(
        jnp.logical_and(is_root, functools.reduce(
            jnp.logical_or, [plane_me == e for e in EARLY])),
        jnp.logical_and(first, functools.reduce(
            jnp.logical_or, [place == n for n in DIRECT_GUESTS])))

    for q in range(4):
        pltpu.make_async_copy(sol_hbm.at[q % 2, q // 2], sol.at[q],
                              sol_sem.at[q // 3]).start()
    def start_eig():
        for q in range(4):
            pltpu.make_async_copy(eig_hbm.at[q % 2, q // 2], eig.at[q % 2, q // 2],
                                  eig_sem).start()

    eager = jnp.logical_or(y < SLOW_LO, y > SLOW_HI)

    @pl.when(eager)
    def _():
        start_eig()

    int_loads = [pltpu.make_async_copy(times_hbm, times_ref, int_sem.at[0]),
                 pltpu.make_async_copy(spin_hbm, spin_ref, int_sem.at[1])]
    for copy in int_loads:
        copy.start()

    def at_place(n):
        return {"z": n // NC, "core": 1 - lax.rem(n, NC)}

    def plane_at(d):
        return {"xh": d // (NY * NXL), "y": d // NXL % NY, "xl": d % NXL, "z": 0, "core": 1}

    def guest(n):
        return {"xh": 0, "y": 0, "xl": 0, "z": n // NC, "core": 1 - n % NC}

    def plane(d):
        return {"xh": d // (NY * NXL), "y": lax.rem(d // NXL, NY), "xl": lax.rem(d, NXL),
                "z": 0, "core": 1}

    barrier = pltpu.get_barrier_semaphore()

    def greet(device):
        pl.semaphore_signal(barrier, inc=1, device_id=device, device_id_type=MESH)

    @pl.when(xh == 0)
    def _():
        greet({"xh": 1 - xh})

    @pl.loop(me + 1, COLUMN)
    def _(o):
        greet(at_place(me + COLUMN - o))

    @pl.when(is_root)
    def _():
        @pl.loop(1, PLANE)
        def _(i):
            greet(plane(lax.rem(plane_me + i, PLANE)))

    @pl.when(is_guest)
    def _():
        @pl.loop(0, PLANE)
        def _(d):
            greet(plane(d))

    @pl.when(is_early)
    def _():
        @pl.loop(0, DIRECT)
        def _(i):
            n = FAR_LO + lax.rem(i, FAR)
            greet({"xh": i // (NXL * FAR_YS * FAR), "xl": lax.rem(i // (FAR_YS * FAR), NXL),
                   "y": FAR_Y + lax.rem(i // FAR, FAR_YS),
                   "z": n // NC, "core": 1 - lax.rem(n, NC)})

    for ref in (high, low):
        for t in range(2):
            for p in range(2):
                ref[t, 128 * p + 96:128 * p + 128] = jnp.zeros((32, 1536), BF16)

    def enter():
        pl.semaphore_wait(barrier, me + xh + jnp.where(is_root, PLANE - 1 + GUESTS, 0)
                          + jnp.where(is_far, len(EARLY) + len(DIRECT_GUESTS), 0))

    def announce():
        @pl.loop(0, me)
        def _(o):
            pl.semaphore_signal(ready, inc=1, device_id=at_place(o), device_id_type=MESH)

        @pl.when(xh == 1)
        def _():
            pl.semaphore_signal(ready, inc=1, device_id={"xh": 1 - xh}, device_id_type=MESH)

    prompt = jnp.logical_and(jnp.logical_not(first), place < PROMPT)
    patient = jnp.logical_and(jnp.logical_not(first), place >= PROMPT)

    @pl.when(prompt)
    def _():
        enter()
        announce()

    squares = jnp.zeros((24, 4, 512), F32)

    def arrived(buf, count, sem):
        pltpu.make_async_copy(buf.at[pl.ds(0, count)], buf.at[pl.ds(0, count)], sem).wait()

    for q in range(4):
        if q == 0:
            arrived(sol, 3, sol_sem.at[0])
        if q == 3:
            arrived(sol, 1, sol_sem.at[1])
        for c in range(3):
            piece = sol[q, :, c]
            squares = squares + piece * piece

    lanes = (squares[:, :, :128] + squares[:, :, 128:256]) + (squares[:, :, 256:384] + squares[:, :, 384:])
    sums = jnp.sum(lanes.reshape(96, 128), axis=1, keepdims=True)
    line = lax.broadcasted_iota(jnp.int32, (96, 128), 0)
    spot = lax.broadcasted_iota(jnp.int32, (96, 128), 1)
    row[...] = jnp.sum(jnp.where(line // 4 == spot, sums, F32(0)), axis=0, keepdims=True)

    def send_row(slot, sem, device):
        pltpu.make_async_remote_copy(
            src_ref=row, dst_ref=slot, send_sem=ssem, recv_sem=sem,
            device_id=device, device_id_type=MESH).start()

    @pl.when(patient)
    def _():
        enter()

    @pl.when(is_far)
    def _():
        spot = ((xh * NXL + xl) * FAR_YS + y - FAR_Y) * FAR + place - FAR_LO
        send_row(rows3.at[pl.ds(spot, 1)], rsem.at[4], plane_at(EARLY[0]))
        send_row(rows1.at[pl.ds(me, 1)], rsem.at[4], {"z": 0, "core": 1})
        for n in DIRECT_GUESTS:
            send_row(rows3.at[pl.ds(spot, 1)], rsem.at[4], guest(n))
        for e in EARLY[1:]:
            send_row(rows3.at[pl.ds(spot, 1)], rsem.at[4], plane_at(e))

    @pl.when(jnp.logical_not(functools.reduce(jnp.logical_or, [is_root, is_far, first])))
    def _():
        send_row(rows1.at[pl.ds(me, 1)], rsem.at[0], {"z": 0, "core": 1})

    @pl.when(patient)
    def _():
        announce()

    @pl.when(jnp.logical_not(eager))
    def _():
        start_eig()

    for t in range(2):
        for p in range(2):
            for c in range(3):
                h, l = split(sol[2 * t + p, :, c].reshape(96, 512))
                high[t, 128 * p:128 * p + 96, 512 * c:512 * c + 512] = h
                low[t, 128 * p:128 * p + 96, 512 * c:512 * c + 512] = l

    for copy in int_loads:
        copy.wait()
    pltpu.make_async_copy(eig, eig, eig_sem).wait()
    lane = lax.broadcasted_iota(jnp.int32, (1, 128), 1)
    lane16 = lax.broadcasted_iota(jnp.int32, (16, 128), 1)
    signs = []
    for t in range(2):
        now = (y * NXL + xl) * 2 + t
        sign = jnp.ones((1, 128), F32)
        for s in range(3):
            edge = jnp.where(now < times_ref[s], F32(-1), F32(1))
            for k in range(8):
                chir = jnp.where(spin_ref[s, k] < 2, F32(1), F32(-1))
                sign = jnp.where(lane // 4 == s * 8 + k, edge * chir, sign)
        signs.append(sign)

    for t in range(2):
        sign = signs[t]
        e = jnp.concatenate(
            [jnp.concatenate([eig[p, t, c] for c in range(3)], axis=1) for p in range(2)], axis=0)
        eh, el = split(e)
        both = dot_rows(jnp.concatenate([eh, el], axis=0), high[t])
        prod = both[:128] + (both[128:] + dot_rows(eh, low[t]))
        real = (prod[:64, :128] + prod[64:, 128:]) * sign
        imag = (prod[:64, 128:] - prod[64:, :128]) * sign
        for p, part in enumerate((real, imag)):
            tmp[:64] = part
            a0 = tmp[pl.ds(0, 16, stride=4), :]
            r1 = pltpu.roll(tmp[pl.ds(1, 16, stride=4), :], 96, 1)
            r2 = pltpu.roll(tmp[pl.ds(2, 16, stride=4), :], 64, 1)
            r3 = pltpu.roll(tmp[pl.ds(3, 16, stride=4), :], 32, 1)
            blocks = (jnp.where(lane16 < 96, a0, r1), jnp.where(lane16 < 64, r1, r2),
                      jnp.where(lane16 < 32, r2, r3))
            for r, block in enumerate(blocks):
                for h in range(2):
                    send[pl.ds(r * 8 + h * 4 + p * 2 + t, 8, stride=24), :] = block[8 * h:8 * h + 8]

    @pl.when(first)
    def _():
        enter()

        @pl.when(jnp.logical_not(is_root))
        def _():
            announce()
            send_row(rows1.at[pl.ds(me, 1)], rsem.at[0], {"z": 0, "core": 1})

    def send_block(o):
        peer = at_place(o)
        spot = pl.multiple_of((peer["z"] * NC + peer["core"]) * 8, 8)
        pltpu.make_async_remote_copy(
            src_ref=send.at[pl.ds(spot, 8)], dst_ref=recv.at[me],
            send_sem=ssem, recv_sem=rsem.at[1],
            device_id=peer, device_id_type=MESH).start()

    @pl.loop(0, me)
    def _(o):
        send_block(o)

    def share(source, device):
        pltpu.make_async_remote_copy(
            src_ref=source, dst_ref=rows2.at[pl.ds(plane_me, 1)], send_sem=ssem, recv_sem=rsem.at[2],
            device_id=device, device_id_type=MESH).start()

    def share_early(source):
        for e in EARLY:
            @pl.when(plane_me != e)
            def _():
                share(source, plane_at(e))

        for n in DIRECT_GUESTS:
            share(source, guest(n))

    is_far_root = jnp.logical_and(is_root, in_far)

    @pl.when(is_root)
    def _():
        rows1[0:1] = row[...]

    @pl.when(is_far_root)
    def _():
        arrived(tally, FAR_LO - 1, rsem.at[0])
        near[...] = jnp.sum(rows1[0:FAR_LO], axis=0, keepdims=True)
        share_early(near)

    @pl.when(jnp.logical_or(me < COLUMN - 1, xh == 0))
    def _():
        pl.semaphore_wait(ready, COLUMN - me - xh)

    @pl.loop(me + 1, COLUMN)
    def _(o):
        send_block(o)

    recv[me] = send[pl.ds(pl.multiple_of((z * NC + core) * 8, 8), 8), :]

    @pl.when(is_far_root)
    def _():
        arrived(tally, FAR, rsem.at[4])
        total[...] = near[...] + jnp.sum(rows1[FAR_LO:COLUMN], axis=0, keepdims=True)

    @pl.when(jnp.logical_and(is_root, jnp.logical_not(in_far)))
    def _():
        arrived(tally, COLUMN - 1, rsem.at[0])
        total[...] = jnp.sum(rows1[0:COLUMN], axis=0, keepdims=True)
        share_early(total)

    @pl.when(is_root)
    def _():
        for n in range(1, GUESTS + 1):
            if n not in DIRECT_GUESTS:
                share(total, guest(n))

        for low_end, high_end in OTHERS:
            @pl.loop(low_end, high_end)
            def _(d):
                @pl.when(d != plane_me)
                def _():
                    share(total, plane(d))

        rows2[pl.ds(plane_me, 1)] = total[...]

    arrived(recv, COLUMN - 1, rsem.at[1])
    block = jnp.sum(recv[...], axis=0)
    half[0] = block[:4]
    half[1] = block[4:]
    cross = pltpu.make_async_remote_copy(
        src_ref=half.at[1 - xh], dst_ref=other, send_sem=ssem, recv_sem=rsem.at[3],
        device_id={"xh": 1 - xh}, device_id_type=MESH)
    cross.start()
    cross.wait_recv()
    mine = half[xh] + other[...]
    out_ref[0] = mine[:2]
    out_ref[1] = mine[2:]

    def down(n):
        return pltpu.make_async_remote_copy(
            src_ref=final, dst_ref=final, send_sem=ssem, recv_sem=rsem.at[0],
            device_id=at_place(n), device_id_type=MESH)

    @pl.when(is_root)
    def _():
        arrived(tally, PLANE - 1, rsem.at[2])

    @pl.when(is_guest)
    def _():
        arrived(tally, PLANE, rsem.at[2])

    summing = jnp.logical_or(is_root, is_guest)

    @pl.when(summing)
    def _():
        final[...] = jnp.sum(rows2[...], axis=0, keepdims=True)

    @pl.when(is_early)
    def _():
        arrived(tally, DIRECT, rsem.at[4])
        final[...] = final[...] + jnp.sum(rows3[...], axis=0, keepdims=True)

    @pl.when(jnp.logical_not(summing))
    def _():
        down(0).wait_recv()

    plain_root = jnp.logical_and(is_root, jnp.logical_not(first))

    @pl.when(plain_root)
    def _():
        for n in range(1, RELAY + 1):
            down(n).start()

    @pl.when(is_relay)
    def _():
        @pl.loop(RELAY + 1, COLUMN)
        def _(n):
            down(n).start()

    @pl.when(is_spare)
    def _():
        @pl.loop(GUESTS + 1, COLUMN)
        def _(n):
            down(n).start()

    norm = final[...] * F32(1 / 9437184.0)
    for s in range(3):
        norm_ref[s:s + 1, :] = pltpu.roll(norm, (128 - 8 * s) % 128, 1)[:, :8]

    base = 8 * (COLUMN - 1) + 4
    roles = ((jnp.logical_and(is_root, first), PLANE - 1 + GUESTS),
             (plain_root, PLANE - 1 + GUESTS + RELAY),
             (is_relay, COLUMN - RELAY),
             (is_spare, COLUMN - GUESTS),
             (is_far, 1 + len(EARLY) + len(DIRECT_GUESTS)))
    rest = True
    for role, count in roles:
        pl.when(role)(functools.partial(arrived, tally, base + count, ssem))
        rest = jnp.logical_and(rest, jnp.logical_not(role))
    pl.when(rest)(functools.partial(arrived, tally, base + 1, ssem))


def finish(block_ref, norm_ref, block_out, norm_out, sem):
    copies = [pltpu.make_async_copy(block_ref, block_out, sem.at[0]),
              pltpu.make_async_copy(norm_ref, norm_out, sem.at[1])]
    for copy in copies:
        copy.start()
    for copy in copies:
        copy.wait()


def on_device(eigvecs, solutions, source_times, spin_dilution):
    eig = jnp.transpose(eigvecs, (0, 1, 3, 2, 4))
    sol = jnp.transpose(solutions, (0, 1, 2, 3, 5, 4, 6)).reshape(2, 2, 24, 3, 4, 512)
    vmem = pl.BlockSpec(memory_space=pltpu.VMEM)
    hbm = pl.BlockSpec(memory_space=pl.ANY)
    results = (jax.ShapeDtypeStruct((2, 2, 128), F32), jax.ShapeDtypeStruct((3, 8), F32))
    block, norm = pl.pallas_call(
        kernel,
        out_shape=(pltpu.VMEM((2, 2, 128), F32), pltpu.VMEM((3, 8), F32)),
        in_specs=[hbm, hbm, hbm, hbm],
        out_specs=(vmem, vmem),
        scratch_shapes=[
            pltpu.VMEM((2, 2, 3, 64, 512), F32),
            pltpu.VMEM((4, 24, 3, 4, 512), F32),
            pltpu.SMEM((3,), jnp.int32),
            pltpu.SMEM((3, 8), jnp.int32),
            pltpu.VMEM((2, 256, 1536), BF16),
            pltpu.VMEM((2, 256, 1536), BF16),
            pltpu.VMEM((72, 128), F32),
            pltpu.VMEM((COLUMN * 8 + 24, 128), F32),
            pltpu.VMEM((COLUMN, 8, 128), F32),
            pltpu.VMEM((2, 4, 128), F32),
            pltpu.VMEM((4, 128), F32),
            pltpu.VMEM((1, 128), F32),
            pltpu.VMEM((COLUMN, 128), F32),
            pltpu.VMEM((1, 128), F32),
            pltpu.VMEM((1, 128), F32),
            pltpu.VMEM((PLANE, 128), F32),
            pltpu.VMEM((DIRECT, 128), F32),
            pltpu.VMEM((1, 128), F32),
            pltpu.VMEM((256, 1, 128), F32),
            pltpu.SemaphoreType.DMA((2,)),
            pltpu.SemaphoreType.DMA,
            pltpu.SemaphoreType.DMA((2,)),
            pltpu.SemaphoreType.DMA,
            pltpu.SemaphoreType.DMA((5,)),
            pltpu.SemaphoreType.REGULAR,
        ],
        compiler_params=pltpu.CompilerParams(collective_id=0, has_side_effects=True),
        name="perambulator",
    )(source_times, spin_dilution, eig, sol)
    return pl.pallas_call(
        finish,
        out_shape=results,
        in_specs=[vmem, vmem],
        out_specs=(hbm, hbm),
        scratch_shapes=[pltpu.SemaphoreType.DMA((2,))],
        compiler_params=pltpu.CompilerParams(vmem_limit_bytes=1 << 20),
        name="finish",
    )(pltpu.with_memory_space_constraint(block, pltpu.VMEM),
      pltpu.with_memory_space_constraint(norm, pltpu.VMEM))


def solution(mesh):
    finer = Mesh(mesh.devices.reshape(NY, NXL, NXH, NZ, NC), TA + SA)
    return jax.shard_map(
        on_device,
        mesh=finer,
        in_specs=(P(None, TA, None, None, SA), P(None, TA, None, None, None, None, SA), P(), P()),
        out_specs=(P(None, TA, SA), P()),
        check_vma=False,
    )
```
